8 devices in a mesh: fsdp: 8 (over z, y, x, core).
Axes of the slice: x: 2, y: 2, z: 1, core: 2. Of those that a mesh axis runs over, the one named last changes fastest.
Arguments:
- act_in: bfloat16 [256, 196, 1024], P('fsdp')
- labels: int32 [256], P('fsdp')
- layer_p: float32 [2, 8599552], P(None, 'fsdp')
- head_w: float32 [1024, 21843], P('fsdp')
- small_p: float32 [24576], P('fsdp')
- layer_m: float32 [2, 8599552], P(None, 'fsdp')
- head_m: float32 [1024, 21843], P('fsdp')
- small_m: float32 [24576], P('fsdp')
- layer_v: float32 [2, 8599552], P(None, 'fsdp')
- head_v: float32 [1024, 21843], P('fsdp')
- small_v: float32 [24576], P('fsdp')
Outputs:
- output 1: float32 [], replicated
- output 2: float32 [2, 8599552], P(None, 'fsdp')
- output 3: float32 [1024, 21843], P('fsdp')
- output 4: float32 [24576], P('fsdp')
- output 5: float32 [2, 8599552], P(None, 'fsdp')
- output 6: float32 [1024, 21843], P('fsdp')
- output 7: float32 [24576], P('fsdp')
- output 8: float32 [2, 8599552], P(None, 'fsdp')
- output 9: float32 [1024, 21843], P('fsdp')
- output 10: float32 [24576], P('fsdp')
All inputs are finite; a program needn't handle non-finite values.
Results may differ from the reference program's by a relative error of at most 0.001.
Values are sent between devices in bfloat16 or wider.
A program may use at most 1 GiB of HBM per device.

```python
import jax
import jax.numpy as jnp
from jax import lax

CHANNELS = 1024
TOKENS = 196
TOKEN_HID = 512
CHAN_HID = 4096
CLASSES = 21843
BATCH_DEV = 32
FSDP_DEVS = 8
ADAM_STEP = 10

GLOBAL_BATCH = BATCH_DEV * FSDP_DEVS
PAD_UNIT = 128 * FSDP_DEVS
MAT_LEN = 2 * TOKENS * TOKEN_HID + 2 * CHANNELS * CHAN_HID
LAYER_LEN = MAT_LEN + 5 * CHANNELS + TOKEN_HID + TOKENS + CHAN_HID
LAYER_PAD = (LAYER_LEN + PAD_UNIT - 1) // PAD_UNIT * PAD_UNIT
SMALL_LEN = 2 * CHANNELS + CLASSES
SMALL_PAD = (SMALL_LEN + PAD_UNIT - 1) // PAD_UNIT * PAD_UNIT
PIECE_SIZES = (TOKENS * TOKEN_HID, TOKEN_HID * TOKENS, CHANNELS * CHAN_HID, CHAN_HID * CHANNELS, CHANNELS, CHANNELS, TOKEN_HID, TOKENS, CHANNELS, CHANNELS, CHAN_HID, CHANNELS)
LN_EPS = 1e-6
LEARN_RATE = 0.003
BETA_ONE = 0.9
BETA_TWO = 0.999
ADAM_EPS = 1e-8
WEIGHT_DECAY = 0.03


def unpack_layer(flat):
    pieces = []
    piece_start = 0
    for piece_len in PIECE_SIZES:
        pieces.append(flat[piece_start:piece_start + piece_len])
        piece_start = piece_start + piece_len
    w_tok1 = pieces[0].reshape(TOKENS, TOKEN_HID)
    w_tok2 = pieces[1].reshape(TOKEN_HID, TOKENS)
    w_ch1 = pieces[2].reshape(CHANNELS, CHAN_HID)
    w_ch2 = pieces[3].reshape(CHAN_HID, CHANNELS)
    return [w_tok1, w_tok2, w_ch1, w_ch2] + pieces[4:12]


def layer_norm(x_in, ln_gain, ln_shift):
    x_f = x_in.astype(jnp.float32)
    mean_val = jnp.mean(x_f, axis=-1, keepdims=True)
    var_val = jnp.mean(jnp.square(x_f - mean_val), axis=-1, keepdims=True)
    normed = (x_f - mean_val) * lax.rsqrt(var_val + LN_EPS)
    return (normed * ln_gain.astype(jnp.float32) + ln_shift.astype(jnp.float32)).astype(jnp.bfloat16)


def mixer_layer(x_in, flat):
    w_tok1, w_tok2, w_ch1, w_ch2, ln1_g, ln1_b, b_tok1, b_tok2, ln2_g, ln2_b, b_ch1, b_ch2 = unpack_layer(flat)
    normed = layer_norm(x_in, ln1_g, ln1_b)
    hid_tok = jnp.einsum('bsc,sj->bcj', normed.astype(jnp.float32), w_tok1.astype(jnp.float32)) + b_tok1.astype(jnp.float32)
    act_tok = jax.nn.gelu(hid_tok).astype(jnp.bfloat16)
    tok_out = jnp.einsum('bcj,js->bsc', act_tok.astype(jnp.float32), w_tok2.astype(jnp.float32)) + b_tok2.astype(jnp.float32)[:, None]
    after_tok = (x_in.astype(jnp.float32) + tok_out).astype(jnp.bfloat16)
    normed2 = layer_norm(after_tok, ln2_g, ln2_b)
    hid_ch = jnp.einsum('bsc,cd->bsd', normed2.astype(jnp.float32), w_ch1.astype(jnp.float32)) + b_ch1.astype(jnp.float32)
    act_ch = jax.nn.gelu(hid_ch).astype(jnp.bfloat16)
    ch_out = jnp.einsum('bsd,dc->bsc', act_ch.astype(jnp.float32), w_ch2.astype(jnp.float32)) + b_ch2.astype(jnp.float32)
    return (after_tok.astype(jnp.float32) + ch_out).astype(jnp.bfloat16)


def block_loss(layer_p, head_w, small_p, x_block, label_block):
    layers_bf = layer_p.astype(jnp.bfloat16)
    hidden = x_block
    for layer_idx in range(2):
        hidden = mixer_layer(hidden, layers_bf[layer_idx])
    small_bf = small_p.astype(jnp.bfloat16)
    lnf_g = small_bf[:CHANNELS]
    lnf_b = small_bf[CHANNELS:2 * CHANNELS]
    head_b = small_bf[2 * CHANNELS:2 * CHANNELS + CLASSES]
    normed = layer_norm(hidden, lnf_g, lnf_b)
    pooled = jnp.mean(normed.astype(jnp.float32), axis=1).astype(jnp.bfloat16)
    logits = jnp.dot(pooled, head_w.astype(jnp.bfloat16), preferred_element_type=jnp.float32) + head_b.astype(jnp.float32)
    log_norm = jax.nn.logsumexp(logits, axis=-1)
    is_label = jnp.arange(CLASSES)[None, :] == label_block[:, None]
    picked = jnp.sum(jnp.where(is_label, logits, 0.0), axis=-1)
    return jnp.sum(log_norm - picked) / GLOBAL_BATCH


def loss_and_grads(act_in, labels, layer_p, head_w, small_p):
    x_blocks = act_in.reshape(FSDP_DEVS, BATCH_DEV, TOKENS, CHANNELS)
    label_blocks = labels.reshape(FSDP_DEVS, BATCH_DEV)
    grad_fn = jax.value_and_grad(block_loss, argnums=(0, 1, 2))

    def scan_body(running, block_pair):
        loss_part, grad_parts = grad_fn(layer_p, head_w, small_p, block_pair[0], block_pair[1])
        return (running[0] + loss_part, running[1] + grad_parts[0], running[2] + grad_parts[1], running[3] + grad_parts[2]), None

    start_val = (jnp.zeros((), jnp.float32), jnp.zeros_like(layer_p), jnp.zeros_like(head_w), jnp.zeros_like(small_p))
    totals, _ = lax.scan(scan_body, start_val, (x_blocks, label_blocks))
    return totals


def adam_update(master, gradient, moment, second, decay_rate):
    moment_new = BETA_ONE * moment + (1.0 - BETA_ONE) * gradient
    second_new = BETA_TWO * second + (1.0 - BETA_TWO) * gradient * gradient
    m_hat = moment_new / (1.0 - BETA_ONE ** ADAM_STEP)
    v_hat = second_new / (1.0 - BETA_TWO ** ADAM_STEP)
    master_new = master - LEARN_RATE * (m_hat / (jnp.sqrt(v_hat) + ADAM_EPS) + decay_rate * master)
    return master_new, moment_new, second_new


def draw_layer(key):
    subkeys = jax.random.split(key, 13)
    normal = jax.random.normal
    pieces = [
        normal(subkeys[0], (TOKENS * TOKEN_HID,), jnp.float32) * TOKENS ** -0.5,
        normal(subkeys[1], (TOKEN_HID * TOKENS,), jnp.float32) * TOKEN_HID ** -0.5,
        normal(subkeys[2], (CHANNELS * CHAN_HID,), jnp.float32) * CHANNELS ** -0.5,
        normal(subkeys[3], (CHAN_HID * CHANNELS,), jnp.float32) * CHAN_HID ** -0.5,
        1.0 + 0.2 * normal(subkeys[4], (CHANNELS,), jnp.float32),
        0.2 * normal(subkeys[5], (CHANNELS,), jnp.float32),
        0.3 * normal(subkeys[6], (TOKEN_HID,), jnp.float32),
        0.3 * normal(subkeys[7], (TOKENS,), jnp.float32),
        1.0 + 0.2 * normal(subkeys[8], (CHANNELS,), jnp.float32),
        0.2 * normal(subkeys[9], (CHANNELS,), jnp.float32),
        0.3 * normal(subkeys[10], (CHAN_HID,), jnp.float32),
        0.3 * normal(subkeys[11], (CHANNELS,), jnp.float32),
        0.02 * normal(subkeys[12], (LAYER_PAD - LAYER_LEN,), jnp.float32),
    ]
    return jnp.concatenate(pieces)


def setup_inputs(seed: int = 0) -> dict:
    keys = jax.random.split(jax.random.key(seed), 12)
    normal = jax.random.normal
    base = normal(keys[0], (GLOBAL_BATCH, 1, CHANNELS), jnp.float32)
    noise = normal(keys[1], (GLOBAL_BATCH, TOKENS, CHANNELS), jnp.float32)
    act_in = (base + noise).astype(jnp.bfloat16)
    labels = jax.random.randint(keys[2], (GLOBAL_BATCH,), 0, CLASSES, jnp.int32)
    layer_p = jnp.stack([draw_layer(keys[3]), draw_layer(keys[4])])
    head_w = normal(keys[5], (CHANNELS, CLASSES), jnp.float32) * CHANNELS ** -0.5
    small_p = jnp.concatenate([
        2.0 + 0.3 * normal(keys[6], (CHANNELS,), jnp.float32),
        0.3 * normal(keys[7], (CHANNELS,), jnp.float32),
        normal(keys[8], (CLASSES,), jnp.float32),
        0.02 * normal(keys[9], (SMALL_PAD - SMALL_LEN,), jnp.float32),
    ])
    _, g_layer, g_head, g_small = loss_and_grads(act_in, labels, layer_p, head_w, small_p)
    layer_rms = jnp.sqrt(jnp.mean(jnp.square(g_layer), axis=1, keepdims=True))
    head_rms = jnp.sqrt(jnp.mean(jnp.square(g_head)))
    small_rms = jnp.sqrt(jnp.mean(jnp.square(g_small)))
    mkeys = jax.random.split(keys[10], 6)
    uniform = jax.random.uniform
    layer_m = 0.3 * layer_rms * normal(mkeys[0], layer_p.shape, jnp.float32)
    head_m = 0.3 * head_rms * normal(mkeys[1], head_w.shape, jnp.float32)
    small_m = 0.3 * small_rms * normal(mkeys[2], small_p.shape, jnp.float32)
    layer_v = 0.01 * jnp.square(layer_rms) * uniform(mkeys[3], layer_p.shape, jnp.float32, 0.5, 2.0)
    head_v = 0.01 * jnp.square(head_rms) * uniform(mkeys[4], head_w.shape, jnp.float32, 0.5, 2.0)
    small_v = 0.01 * jnp.square(small_rms) * uniform(mkeys[5], small_p.shape, jnp.float32, 0.5, 2.0)
    return {'act_in': act_in, 'labels': labels, 'layer_p': layer_p, 'head_w': head_w, 'small_p': small_p, 'layer_m': layer_m, 'head_m': head_m, 'small_m': small_m, 'layer_v': layer_v, 'head_v': head_v, 'small_v': small_v}


def reference(act_in, labels, layer_p, head_w, small_p, layer_m, head_m, small_m, layer_v, head_v, small_v):
    loss_value, g_layer, g_head, g_small = loss_and_grads(act_in, labels, layer_p, head_w, small_p)
    sq_total = jnp.sum(jnp.square(g_layer)) + jnp.sum(jnp.square(g_head)) + jnp.sum(jnp.square(g_small))
    clip_scale = 1.0 / jnp.maximum(1.0, jnp.sqrt(sq_total))
    layer_decay = jnp.where(jnp.arange(LAYER_PAD) < MAT_LEN, WEIGHT_DECAY, 0.0)[None, :]
    new_lp, new_lm, new_lv = adam_update(layer_p, g_layer * clip_scale, layer_m, layer_v, layer_decay)
    new_hw, new_hm, new_hv = adam_update(head_w, g_head * clip_scale, head_m, head_v, WEIGHT_DECAY)
    new_sp, new_sm, new_sv = adam_update(small_p, g_small * clip_scale, small_m, small_v, 0.0)
    return (loss_value, new_lp, new_hw, new_sp, new_lm, new_hm, new_sm, new_lv, new_hv, new_sv)
```

```python
import functools
import math
import jax
import jax.numpy as jnp
from jax import lax
from jax.experimental import pallas as pl
from jax.experimental.pallas import tpu as pltpu
from jax.experimental.layout import with_layout_constraint, Layout
from jax.sharding import PartitionSpec as P


F32 = jnp.float32
BF = jnp.bfloat16
LN_EPS = 1e-6
LEARN_RATE = 0.003
BETA_ONE = 0.9
BETA_TWO = 0.999
ADAM_EPS = 1e-8
WEIGHT_DECAY = 0.03
ADAM_STEP = 10
GC0 = math.sqrt(2 / math.pi)
GC1 = GC0 * 0.044715

LANE = 128
SUB = 8
ND = 8
AX = 'fsdp'
B = 32
S = 196
SP = 200
C = 1024
J = 512
D = 4096
NCLS = 21843
NIMG = 256
T = B * SP
KC = 2816
KR = KC // LANE
RSH = 8398
TOKR = 1568
HTOK = TOKR // 2
UNIT = 512
NU = 16
UR = UNIT * NU
STEPR = RSH - UR
SPILL = TOKR - STEPR
SPR = SPILL + 6
MATR = TOKR + ND * UR
SMR = 80
GROWS = RSH + SPILL + SUB
TP = 208
SMF = 192
SMD = SMF // ND
VROW = 16
VLIM = 64 * 1024 * 1024 - 65536
NT = (((1,), (1,)), ((), ()))
TN = (((0,), (0,)), ((), ()))
VM = pl.BlockSpec(memory_space=pltpu.VMEM)
HBM = pl.BlockSpec(memory_space=pl.ANY)
SMEM = pl.BlockSpec(memory_space=pltpu.SMEM)
SEM = pltpu.SemaphoreType.DMA
VG1, VS1, VG2, VS2, VB2, VB1, VLG, VLS = 0, 1, 2, 3, 4, 5, 9, 10


ZERO, ONE, TWO, THREE, FOUR, TEN = 0, 1, 2, 3, 4, 10


def sds(shape, dt):
    return jax.ShapeDtypeStruct(shape, dt)


def fixed(shape, idx=None, once=False):
    ix = tuple(idx) if idx else (0,) * len(shape)
    return pl.BlockSpec(shape, lambda i: ix, pipeline_mode=pl.Buffered(1) if once else None)


def run(body, ins, in_specs, outs, out_specs, scratch=(), grid=None, flops=10**9, nbytes=10**6, alias={}, cid=None, vlim=VLIM):
    kw = dict(vmem_limit_bytes=vlim)
    if cid is not None:
        kw.update(collective_id=cid, has_side_effects=True)
    if grid:
        kw.update(dimension_semantics=("arbitrary",))
    extra = dict(grid=(grid,)) if grid else {}
    return pl.pallas_call(body, in_specs=in_specs, out_specs=out_specs, out_shape=outs, scratch_shapes=list(scratch),
        input_output_aliases=alias, cost_estimate=pl.CostEstimate(flops=flops, bytes_accessed=nbytes, transcendentals=0),
        compiler_params=pltpu.CompilerParams(**kw), **extra)(*ins)


def on(cond):
    return pl.when(cond)


def unit_stats(xf):
    mean = jnp.sum(xf, axis=-ONE, keepdims=True) * (1.0 / C)
    xc = xf - mean
    rstd = lax.rsqrt(jnp.sum(xc * xc, axis=-ONE, keepdims=True) * (1.0 / C) + LN_EPS)
    return xc * rstd, rstd


def sum8(v):
    return jnp.sum(v.reshape(v.shape[ZERO] // SUB, SUB, v.shape[ONE]), axis=ZERO)


def ln_bwd(nh, rstd, dy, g):
    dxh = dy * g
    m1 = jnp.sum(dxh, axis=-ONE, keepdims=True) * (1.0 / C)
    m2 = jnp.sum(dxh * nh, axis=-ONE, keepdims=True) * (1.0 / C)
    return rstd * (dxh - m1 - nh * m2)


def gelu_both(h):
    u = h * h
    t = jnp.tanh(h * (GC0 + GC1 * u))
    cdf = 0.5 + 0.5 * t
    a = h * cdf
    return a.astype(BF), cdf + (a * (1.0 - t)) * (GC0 + (THREE * GC1) * u)


def wcols(w_ref, c0, n):
    r = w_ref.shape[ZERO] * 16
    return jnp.concatenate([w_ref[:, j].reshape(r, LANE) for j in range(c0 // LANE, (c0 + n) // LANE)], axis=ONE)


def wrows(w_ref, r0, n):
    return jnp.concatenate([w_ref[r0 // 16:(r0 + n) // 16, j].reshape(n, LANE) for j in range(w_ref.shape[ONE])], axis=ONE)


def dot(a, b):
    return jnp.dot(a, b, preferred_element_type=F32)


def dotg(a, b, dn):
    return lax.dot_general(a, b, dn, preferred_element_type=F32)


def entry_barrier():
    me = lax.axis_index(AX)
    b = pltpu.get_barrier_semaphore()
    for d in range(ONE, ND):
        pl.semaphore_signal(b, inc=ONE, device_id=(lax.rem(me + d, ND),), device_id_type=pl.DeviceIdType.MESH)
    pl.semaphore_wait(b, ND - ONE)
    return me


def rcopy(src, dst, ss, rs, dev):
    return pltpu.make_async_remote_copy(src_ref=src, dst_ref=dst, send_sem=ss, recv_sem=rs, device_id=(dev,), device_id_type=pl.DeviceIdType.MESH)


def ag_all(me, src, dst, ss, rs):
    cs = []
    for d in range(ONE, ND):
        c = rcopy(src, dst.at[me], ss.at[d], rs.at[d], lax.rem(me + d, ND))
        c.start()
        cs.append(c)
    return cs


def wait_all(cs):
    for c in cs:
        c.wait()


def rows3(a):
    b = with_layout_constraint(a.reshape(TWO, RSH, LANE), Layout(major_to_minor=(ONE, ZERO, TWO)))
    return b.transpose(ONE, ZERO, TWO)


def unrows3(a):
    b = with_layout_constraint(a.transpose(ONE, ZERO, TWO), Layout(major_to_minor=(ONE, ZERO, TWO)))
    return b.reshape(TWO, RSH * LANE)


def start_kernel(p_ref, misc_ref, o0_ref, o1_ref, tok_o, sm_o, misc_o, buf, shs, shr, toks, sms, ds1, ds2, ss_m, rs_m, ss_s, rs_s, ss_t, rs_t, ss_u, ss_h, rs_h):
    c1 = pltpu.make_async_copy(p_ref.at[:TOKR], buf.at[:TOKR], ds1)
    c1.start()
    c2 = pltpu.make_async_copy(p_ref.at[TOKR:], buf.at[TOKR:RSH], ds2)
    c2.start()
    me = entry_barrier()
    csm = ag_all(me, misc_ref, misc_o, ss_m, rs_m)
    misc_o[me] = misc_ref[:]
    c1.wait()
    shs[:] = buf[:SPILL].astype(BF)
    sh = rcopy(shs, shr, ss_h, rs_h, lax.rem(me + ND - ONE, ND))
    sh.start()
    q4 = TOKR // FOUR

    def first_send(d):
        return rcopy(toks.at[d], tok_o.at[d], ss_t.at[d], rs_t.at[d], d)

    def zero_send(d):
        return rcopy(toks.at[ZERO], tok_o.at[ZERO], ss_u.at[d], rs_t.at[ZERO], d)

    def piece(q, d):
        return rcopy(tok_o.at[q], tok_o.at[q], ss_t.at[d], rs_t.at[q], lax.rem(me - ONE + d, ND - ONE) + ONE)

    def small(d):
        return rcopy(sms, sm_o, ss_s.at[d], rs_s, d)

    @on(me == ZERO)
    def _():
        for l in range(TWO):
            for q in range(FOUR):
                toks[FOUR * l + q] = buf[q4 * q:q4 * (q + ONE), l, :].astype(BF)
        for d in range(ONE, ND):
            first_send(d).start()
        for d in range(ONE, ND):
            zero_send(d).start()
        tok_o[:] = toks[:]

    c2.wait()

    @on(me == ND - ONE)
    def _():
        for l in range(TWO):
            sms[l] = buf[RSH - SMR:RSH, l, :].astype(BF)
        for d in range(ND - ONE):
            small(d).start()
        sm_o[:] = sms[:]

    off = TOKR - STEPR * me

    def go(o_ref, l, nj, a, b):
        n = UNIT // nj // 16

        def step(i, _):
            for j in range(nj):
                o_ref[i * nj + j] = buf[pl.ds(off + i * 16 * nj + j, 16, stride=nj), l, :].astype(BF)
            return ZERO

        lax.fori_loop(a * n, b * n, step, ZERO)

    def both(l, a, b):
        o_ref = (o0_ref, o1_ref)[l]

        @on(me < ND // TWO)
        def _():
            go(o_ref, l, D // LANE, a, b)

        @on(me >= ND // TWO)
        def _():
            go(o_ref, l, C // LANE, a, b)

    own = NU - THREE
    both(ZERO, ZERO, own)

    @on(me > ZERO)
    def _():
        piece(me, ZERO).wait_recv()
        for d in range(ONE, ND - ONE):
            piece(me, d).start()

    both(ONE, ZERO, own)
    sh.wait()
    buf[RSH:RSH + SPILL] = shr[:].astype(F32)
    both(ZERO, own, NU)
    both(ONE, own, NU)
    wait_all(csm)

    @on(me < ND - ONE)
    def _():
        small(ZERO).wait_recv()

    @on(me > ZERO)
    def _():
        for d in range(ND - ONE):
            piece(lax.rem(me + ONE + d, ND), ZERO).wait_recv()
        for d in range(ONE, ND - ONE):
            piece(me, d).wait_send()

    @on(me == ZERO)
    def _():
        for d in range(ONE, ND):
            first_send(d).wait_send()
            zero_send(d).wait_send()

    @on(me == ND - ONE)
    def _():
        for d in range(ND - ONE):
            small(d).wait_send()


def start(p3, misc, cid):
    n = (ND,)
    return run(start_kernel, (p3, misc), [HBM, VM],
        [sds((UNIT, 16, LANE), BF)] * TWO + [sds((ND, TOKR // FOUR, LANE), BF), sds((TWO, SMR, LANE), BF), sds(n + misc.shape, F32)], [VM] * 5,
        scratch=[pltpu.VMEM((GROWS, TWO, LANE), F32), pltpu.VMEM((SPILL, TWO, LANE), BF), pltpu.VMEM((SPILL, TWO, LANE), BF),
            pltpu.VMEM((ND, TOKR // FOUR, LANE), BF), pltpu.VMEM((TWO, SMR, LANE), BF), SEM, SEM, SEM(n), SEM(n), SEM(n), SEM, SEM(n), SEM(n), SEM(n), SEM, SEM],
        flops=TEN**TEN, cid=cid)


def shift_pick(a, b, lane, r):
    return jnp.where(lane < LANE - r, pltpu.roll(a, (LANE - r) % LANE, ONE), pltpu.roll(b, (LANE - r) % LANE, ONE))


def wprep_kernel(tok_ref, sm_ref, misc_ref, w1a_ref, w1t_ref, w2p_ref, w2t_ref, b2c_ref, vec_ref, lab_ref, bias_ref, tf, w1s, w2l, w2h, sf, sg):
    me = lax.axis_index(AX)
    for k in range(ND):
        sf[k * SMD:(k + ONE) * SMD, :] = misc_ref[k, :SMD, :].astype(BF).astype(F32)
        lab_ref[:, k * B:(k + ONE) * B] = jnp.broadcast_to(misc_ref[k, SMD:SMD + ONE, :B], (SUB, B))
    bias_ref[:] = jnp.zeros(bias_ref.shape, F32)
    bias_ref[:KR, :] = sf[pl.ds(16 + KR * me, KR), :]
    vec_ref[:] = jnp.zeros(vec_ref.shape, F32)
    w1s[:] = jnp.zeros(w1s.shape, F32)
    lane = lax.broadcasted_iota(jnp.int32, (16, LANE), ONE)

    def put(l, row, src, r0, n):
        for i in range(n):
            vec_ref[l, row + i // SUB:row + i // SUB + ONE, (i % SUB) * LANE:(i % SUB + ONE) * LANE] = src[r0 + i:r0 + i + ONE, :]

    for l in range(TWO):
        for q in range(FOUR):
            tf[q * (TOKR // FOUR):(q + ONE) * (TOKR // FOUR), :] = tok_ref[FOUR * l + q].astype(F32)
        smf = sm_ref[l].astype(F32)
        sg[:SMR, :] = smf
        for j in range(FOUR):
            w1s[:S, j * LANE:(j + ONE) * LANE] = tf[pl.ds(j, S, stride=FOUR), :]
            w1s[S:S + ONE, j * LANE:(j + ONE) * LANE] = sg[16 + j:17 + j, :]
        for b in range(32):
            p = S * b
            r0 = HTOK + p // LANE
            o = p % LANE
            x = [tf[pl.ds(r0 + q, 16, stride=49), :] for q in range(THREE if o + S > TWO * LANE else TWO)]
            w2l[pl.ds(b, 16, stride=32), :] = shift_pick(x[ZERO], x[ONE], lane, o)
            hi = shift_pick(x[ONE], x[-ONE], lane, o)
            w2h[pl.ds(b, 16, stride=32), :] = jnp.where(lane < S - LANE, hi, 0.0)
        w1 = w1s[:]
        w2 = jnp.concatenate([w2l[:], w2h[:]], axis=ONE)
        w1a_ref[l] = w1[:SP].astype(BF)
        w1t_ref[l] = w1.T[:, :SP].astype(BF)
        w2p_ref[l] = w2[:, :SP].astype(BF)
        w2t_ref[l] = w2.T[:SP].astype(BF)
        put(l, VG1, sg, ZERO, SUB)
        put(l, VS1, sg, SUB, SUB)
        b2 = jnp.concatenate([sg[20:21, :], sg[21:22, :]], axis=ONE)
        b2 = jnp.broadcast_to(b2, (SUB, TWO * LANE)).T[:SP, :ONE]
        rowi = lax.broadcasted_iota(jnp.int32, (SP, LANE), ZERO)
        b2c_ref[l] = jnp.where(rowi < S, jnp.broadcast_to(b2, (SP, LANE)), 0.0)
        lane7 = lax.broadcasted_iota(jnp.int32, (56, LANE), ONE)
        sg[:56, :] = shift_pick(smf[21:77], smf[22:78], lane7, S - LANE)
        put(l, VG2, sg, ZERO, SUB)
        put(l, VS2, sg, SUB, SUB)
        put(l, VB1, sg, 16, 32)
        put(l, VB2, sg, 48, SUB)
        put(l, VLG, sf, ZERO, SUB)
        put(l, VLS, sf, SUB, SUB)


def wprep(tok, sm, misc):
    return run(wprep_kernel, (tok, sm, misc), [VM] * THREE,
        [sds((TWO, SP, J), BF), sds((TWO, J, SP), BF), sds((TWO, J, SP), BF), sds((TWO, SP, J), BF), sds((TWO, SP, LANE), F32), sds((TWO, VROW, C), F32), sds((SUB, NIMG), F32), sds((24, LANE), F32)],
        [VM] * 8, scratch=[pltpu.VMEM((TOKR, LANE), F32), pltpu.VMEM((256, J), F32), pltpu.VMEM((J, LANE), F32), pltpu.VMEM((J, LANE), F32), pltpu.VMEM((SMF, LANE), F32), pltpu.VMEM((SMR, LANE), F32)],
        flops=5 * TEN**9)


def vec_spec(l):
    return fixed((ONE, VROW, C), (l, ZERO, ZERO))


def lay(shape, l):
    return fixed((ONE,) + shape, (l, ZERO, ZERO))


CW = 256


def tok_fwd_kernel(x_ref, w1t_ref, w2t_ref, b2_ref, v_ref, out_ref, n2_ref, act_ref, gp_ref, n_s):
    @on(pl.program_id(ZERO) == ZERO)
    def _():
        r = lax.broadcasted_iota(jnp.int32, (SP, C), ZERO)
        for im in range(TWO):
            n_s[im] = jnp.where(r == S, 1.0, 0.0).astype(BF)

    for im in range(TWO):
        xf = x_ref[im, :S, :].astype(F32)
        nh, _ = unit_stats(xf)
        n_s[im, :S, :] = (nh * v_ref[ZERO, VG1:VG1 + ONE, :] + v_ref[ZERO, VS1:VS1 + ONE, :]).astype(BF)
    for im in range(TWO):
        cols = []
        for c in range(ZERO, C, CW):
            cs = slice(c, c + CW)
            a, gp = gelu_both(dot(w1t_ref[ZERO], n_s[im, :, cs]))
            act_ref[im, :, cs] = a
            gp_ref[im, :, cs] = gp
            o = dot(w2t_ref[ZERO], a) + b2_ref[ZERO, :, :ONE]
            cols.append((x_ref[im, :S, cs].astype(F32) + o[:S]).astype(BF))
        x1 = jnp.concatenate(cols, axis=ONE)
        out_ref[im, :S, :] = x1
        nh2, _ = unit_stats(x1.astype(F32))
        n2_ref[im, :S, :] = (nh2 * v_ref[ZERO, VG2:VG2 + ONE, :] + v_ref[ZERO, VS2:VS2 + ONE, :]).astype(BF)
        out_ref[im, S:, :] = jnp.zeros((SP - S, C), BF)
        n2_ref[im, S:, :] = jnp.zeros((SP - S, C), BF)


def img(r, n=C):
    return pl.BlockSpec((TWO, r, n), lambda i: (i, ZERO, ZERO))


def tok_fwd(x, wp, l):
    return run(tok_fwd_kernel, (x, wp[ONE], wp[THREE], wp[FOUR], wp[5]),
        [img(x.shape[ONE]), lay((J, SP), l), lay((SP, J), l), lay((SP, LANE), l), vec_spec(l)],
        [sds((B, SP, C), BF)] * TWO + [sds((B, J, C), BF), sds((B, J, C), F32)], [img(SP)] * TWO + [img(J)] * TWO,
        scratch=[pltpu.VMEM((TWO, SP, C), BF)], grid=B // TWO, flops=60 * TEN**9, nbytes=14 * TEN**7)


def tok_bwd_kernel(need_dx, x_ref, da_ref, act_ref, gp_ref, w1a_ref, w2p_ref, v_ref, *rest):
    if need_dx:
        dx_ref = rest[ZERO]
        rest = rest[ONE:]
    dw1_ref, dw2_ref, db1_ref, db2_ref, dg_ref, ds_ref, n_s, nh_s, dh_s, dn_s = rest

    @on(pl.program_id(ZERO) == ZERO)
    def _():
        for r in (dw1_ref, dw2_ref, db1_ref, db2_ref, dg_ref, ds_ref, n_s):
            r[:] = jnp.zeros(r.shape, r.dtype)

    rs = []
    for im in range(TWO):
        nh, rstd = unit_stats(x_ref[im, :S, :].astype(F32))
        nh_s[im, :S, :] = nh
        rs.append(rstd)
        n_s[:S, im * C:(im + ONE) * C] = (nh * v_ref[ZERO, VG1:VG1 + ONE, :] + v_ref[ZERO, VS1:VS1 + ONE, :]).astype(BF)
    db1 = db1_ref[:]
    for im in range(TWO):
        for c in range(ZERO, C, CW):
            cs = slice(c, c + CW)
            dact = dot(w2p_ref[ZERO], da_ref[im, :, cs]).astype(BF).astype(F32)
            dh = dact * gp_ref[im, :, cs]
            for k in range(ZERO, CW, LANE):
                db1 = db1 + dh[:, k:k + LANE]
            dhb = dh.astype(BF)
            dh_s[:, im * C + c:im * C + c + CW] = dhb
            dn_s[im, :, cs] = dot(w1a_ref[ZERO], dhb)
    db1_ref[:] = db1
    act2 = jnp.concatenate([act_ref[ZERO], act_ref[ONE]], axis=ONE)
    da2 = jnp.concatenate([da_ref[ZERO], da_ref[ONE]], axis=ONE)
    dw2_ref[:] += dotg(act2, da2, NT)
    dw1_ref[:] += dotg(dh_s[:], n_s[:], NT)
    db2 = db2_ref[:]
    s8 = S // SUB * SUB
    for im in range(TWO):
        for k in range(ZERO, C, LANE):
            db2 = db2 + da_ref[im, :, k:k + LANE].astype(F32)
        dn = dn_s[im, :S, :].astype(BF).astype(F32)
        nh = nh_s[im, :S, :]
        pr = dn * nh
        dg_ref[:] += sum8(pr[:s8])
        ds_ref[:] += sum8(dn[:s8])
        dg_ref[:S - s8] += pr[s8:]
        ds_ref[:S - s8] += dn[s8:]
        if need_dx:
            dx = ln_bwd(nh, rs[im], dn, v_ref[ZERO, VG1:VG1 + ONE, :])
            dx_ref[im, :S, :] = (da_ref[im, :S, :].astype(F32) + dx).astype(BF)
            dx_ref[im, S:, :] = jnp.zeros((SP - S, C), BF)
    db2_ref[:] = db2


def tok_bwd(x, da, act, gp, wp, l):
    acc = [(J, SP), (J, SP), (J, LANE), (SP, LANE), (SUB, C), (SUB, C)]
    dx = [sds((B, SP, C), BF)] if l else []
    return run(functools.partial(tok_bwd_kernel, bool(l)), (x, da, act, gp, wp[ZERO], wp[TWO], wp[5]),
        [img(x.shape[ONE]), img(SP), img(J), img(J), lay((SP, J), l), lay((J, SP), l), vec_spec(l)],
        dx + [sds(s, F32) for s in acc], [img(SP)] * len(dx) + [fixed(s) for s in acc],
        scratch=[pltpu.VMEM((SP, TWO * C), BF), pltpu.VMEM((TWO, SP, C), F32), pltpu.VMEM((J, TWO * C), BF), pltpu.VMEM((TWO, SP, C), F32)],
        grid=B // TWO, flops=60 * TEN**9, nbytes=14 * TEN**7)


M = 400
DC = 512


def row(n):
    return pl.BlockSpec((M, n), lambda i: (i, ZERO))


def wspec(h):
    return fixed((64, 32, 16, LANE) if h == ZERO else (256, SUB, 16, LANE), (h, ZERO, ZERO, ZERO), True)


def ch_fwd_kernel(n2_ref, x1_ref, w1_ref, w2_ref, v_ref, x2_ref, act_ref, gp_ref):
    n2 = n2_ref[:]
    for k in range(D // DC):
        ks = slice(k * DC, (k + ONE) * DC)
        r = VB1 + k // TWO
        b = v_ref[ZERO, r:r + ONE, (k % TWO) * DC:(k % TWO + ONE) * DC]
        act_ref[:, ks], gp_ref[:, ks] = gelu_both(dot(n2, wcols(w1_ref, k * DC, DC)) + b)
    for c in range(ZERO, C, CW):
        cs = slice(c, c + CW)
        o = dot(act_ref[:], wcols(w2_ref, c, CW)) + v_ref[ZERO, VB2:VB2 + ONE, cs]
        x2_ref[:, cs] = (x1_ref[:, cs].astype(F32) + o).astype(BF)


def w_views(wg):
    return wg.reshape(128, 32, 16, LANE), wg.reshape(512, SUB, 16, LANE)


def ch_fwd(n2, x1, wg, wp, l):
    return run(ch_fwd_kernel, (n2, x1) + w_views(wg) + (wp[5],), [row(C), row(C), wspec(ZERO), wspec(ONE), vec_spec(l)],
        [sds((T, C), BF), sds((T, D), BF), sds((T, D), F32)], [row(C), row(D), row(D)],
        grid=T // M, flops=FOUR * T * C * D, nbytes=T * D * 6)


def ch_bwd_a_kernel(do_ref, gp_ref, w2_ref, dh_ref, db1_ref, db2_ref):
    @on(pl.program_id(ZERO) == ZERO)
    def _():
        db1_ref[:] = jnp.zeros(db1_ref.shape, F32)
        db2_ref[:] = jnp.zeros(db2_ref.shape, F32)

    do = do_ref[:]
    db2_ref[:] += sum8(do.astype(F32))
    for k in range(D // DC):
        ks = slice(k * DC, (k + ONE) * DC)
        da = dotg(do, wrows(w2_ref, k * DC, DC), NT).astype(BF).astype(F32)
        dh = da * gp_ref[:, ks]
        db1_ref[:, ks] += sum8(dh)
        dh_ref[:, ks] = dh.astype(BF)


def ch_bwd_a(do, gp, wg):
    return run(ch_bwd_a_kernel, (do, gp, w_views(wg)[ONE]), [row(C), row(D), wspec(ONE)],
        [sds((T, D), BF), sds((SUB, D), F32), sds((SUB, C), F32)], [row(D), fixed((SUB, D)), fixed((SUB, C))],
        grid=T // M, flops=TWO * T * C * D, nbytes=T * D * 6)


def ch_bwd_b_kernel(dh_ref, w1_ref, x1_ref, do_ref, v_ref, da_ref, dg_ref, ds_ref, dn_s):
    @on(pl.program_id(ZERO) == ZERO)
    def _():
        dg_ref[:] = jnp.zeros(dg_ref.shape, F32)
        ds_ref[:] = jnp.zeros(ds_ref.shape, F32)

    for c in range(ZERO, C, CW):
        dn_s[:, c:c + CW] = dotg(dh_ref[:], wrows(w1_ref, c, CW), NT)
    dy = dn_s[:].astype(BF).astype(F32)
    nh, rstd = unit_stats(x1_ref[:].astype(F32))
    dx = ln_bwd(nh, rstd, dy, v_ref[ZERO, VG2:VG2 + ONE, :])
    dg_ref[:] += sum8(dy * nh)
    ds_ref[:] += sum8(dy)
    r = lax.rem(lax.broadcasted_iota(jnp.int32, (M, ONE), ZERO), SP)
    da_ref[:] = jnp.where(r < S, do_ref[:].astype(F32) + dx, 0.0).astype(BF)


def ch_bwd_b(dh, wg, x1, do, wp, l):
    return run(ch_bwd_b_kernel, (dh, w_views(wg)[ZERO], x1, do, wp[5]), [row(D), wspec(ZERO), row(C), row(C), vec_spec(l)],
        [sds((T, C), BF)] + [sds((SUB, C), F32)] * TWO, [row(C)] + [fixed((SUB, C))] * TWO,
        scratch=[pltpu.VMEM((M, C), F32)], grid=T // M, flops=TWO * T * C * D, nbytes=T * D * THREE)


def dw2_kernel(a_ref, b_ref, o_ref):
    r = dotg(a_ref[:], b_ref[:], TN)
    for j in range(C // LANE):
        o_ref[ZERO, :, j] = r[:, LANE * j:LANE * (j + ONE)].reshape(DC // SUB, SUB, LANE)


def dw2_call(act, do, h=None):
    q = C // DC
    own = ND // TWO
    full = h is None
    a_spec = pl.BlockSpec((T, DC), (lambda i: (ZERO, i)) if full else (lambda i: (ZERO, q * i + h)))
    o_map = (lambda i: (own + i // q, lax.rem(i, q), ZERO, ZERO, ZERO)) if full else (lambda i: (own + i, ZERO, ZERO, ZERO, ZERO))
    n = C if full else DC
    return run(dw2_kernel, (act, do), [a_spec, fixed((T, C), once=True)],
        sds((ND, n // SUB, SUB, SUB, LANE), F32), pl.BlockSpec((ONE, DC // SUB, SUB, SUB, LANE), o_map),
        grid=D // DC * n // C, flops=TWO * T * n * D, nbytes=T * D * THREE)


def dw1_kernel(*refs):
    a = jnp.concatenate([r[:] for r in refs[:-THREE]], axis=ONE)
    b_ref, _, o_ref = refs[-THREE:]
    r = dotg(a, b_ref[:], TN)
    for j in range(DC // LANE):
        o_ref[:, :, j] = r[:, LANE * j:LANE * (j + ONE)].reshape(o_ref.shape[:TWO] + (SUB, LANE))


def col_spec(k):
    return fixed((T, LANE), (ZERO, k), True)


def dw1_call(n2, dh, g, h=None):
    full = h is None
    own = ND // TWO
    specs = [fixed((T, C), once=True)] if full else [col_spec(TWO * k + h) for k in range(own)]
    rb = 32 if full else 16
    na = len(specs)
    shape = (ND, rb, 32, SUB, LANE)
    return run(dw1_kernel, (n2,) * na + (dh, g.reshape(shape)), specs + [pl.BlockSpec((T, DC), lambda i: (ZERO, i)), HBM],
        sds(shape, F32), pl.BlockSpec((own, rb, DC // LANE, SUB, LANE), lambda i: (ZERO, ZERO, i, ZERO, ZERO)), alias={na + ONE: ZERO},
        grid=D // DC, flops=TWO * T * (rb * 32) * D, nbytes=T * D * THREE)


PI = FOUR


def pimg():
    return pl.BlockSpec((PI, SP, C), lambda i: (i, ZERO, ZERO))


def pvec():
    return pl.BlockSpec((ONE, PI, C), lambda i: (i, ZERO, ZERO))


def pool_kernel(x_ref, v_ref, o_ref):
    for im in range(PI):
        nh, _ = unit_stats(x_ref[im, :S, :].astype(F32))
        n = (nh * v_ref[ZERO, VLG:VLG + ONE, :] + v_ref[ZERO, VLS:VLS + ONE, :]).astype(BF).astype(F32)
        o_ref[ZERO, im:im + ONE, :] = (jnp.sum(n, axis=ZERO, keepdims=True) * (1.0 / S)).astype(BF).astype(F32)


def pool(x2, wp):
    return run(pool_kernel, (x2, wp[5]), [pimg(), vec_spec(ZERO)], sds((B // PI, PI, C), F32), pvec(), grid=B // PI, flops=TEN**TEN, nbytes=T * C * TWO)


def lnf_kernel(x_ref, dp_ref, v_ref, d_ref, dg_ref, ds_ref):
    @on(pl.program_id(ZERO) == ZERO)
    def _():
        dg_ref[:] = jnp.zeros(dg_ref.shape, F32)
        ds_ref[:] = jnp.zeros(ds_ref.shape, F32)

    g = v_ref[ZERO, VLG:VLG + ONE, :]
    for im in range(PI):
        dn = (dp_ref[ZERO, im:im + ONE, :] * (1.0 / S)).astype(BF).astype(F32)
        nh, rstd = unit_stats(x_ref[im, :S, :].astype(F32))
        dxh = dn * g
        m1 = jnp.sum(dxh, axis=-ONE, keepdims=True) * (1.0 / C)
        m2 = jnp.sum(dxh * nh, axis=-ONE, keepdims=True) * (1.0 / C)
        d_ref[im, :S, :] = (rstd * ((dxh - m1) - nh * m2)).astype(BF)
        d_ref[im, S:, :] = jnp.zeros((SP - S, C), BF)
        dg_ref[ZERO:ONE, :] += dn * jnp.sum(nh, axis=ZERO, keepdims=True)
        ds_ref[ZERO:ONE, :] += dn * float(S)


def lnf_bwd(x2, dp, wp):
    return run(lnf_kernel, (x2, dp, wp[5]), [pimg(), pvec(), vec_spec(ZERO)], [sds((B, SP, C), BF), sds((SUB, C), F32), sds((SUB, C), F32)],
        [pimg(), fixed((SUB, C)), fixed((SUB, C))], grid=B // PI, flops=TEN**TEN, nbytes=T * C * FOUR)


HAB = 1408


def hconv_kernel(w_ref, o_ref):
    r = pl.program_id(ZERO) * HAB + lax.broadcasted_iota(jnp.int32, (HAB, LANE), ZERO)
    o_ref[:] = jnp.where(r < NCLS, w_ref[:], 0.0).astype(BF)


def hconv(wt):
    blk = pl.BlockSpec((HAB, LANE), lambda i: (i, ZERO))
    return run(hconv_kernel, (wt,), [blk], sds((ND * KC, LANE), BF), blk, grid=ND * KC // HAB, nbytes=TWO * TEN**7)


def head_kernel(*refs):
    wall_ref, pooled_ref, bias_ref, lab_ref, dl_ref, gb_ref, loss_ref, dpool_ref, pall_ref, w, lg, pb, st, sta, dps, dpr, ws, ss, rs, ss2, rs2, ss3, rs3 = refs
    pb[:] = pooled_ref[:].astype(BF)
    row0 = pl.multiple_of(KC * lax.axis_index(AX), KC)
    cw = [pltpu.make_async_copy(wall_ref.at[r, pl.ds(row0, KC)], w.at[r], ws.at[r]) for r in range(ND)]
    for c in cw:
        c.start()
    me = entry_barrier()
    cs = ag_all(me, pb, pall_ref, ss, rs)
    pall_ref[me] = pb[:]
    wait_all(cs)

    wait_all(cw)
    bt = bias_ref[:].T
    pm = pall_ref[:].reshape(NIMG, C)
    for q in range(KR // TWO):
        n = q * TWO * LANE
        acc = jnp.concatenate([jnp.broadcast_to(bt[:, TWO * q + k:TWO * q + k + ONE], (LANE, NIMG)) for k in range(TWO)], axis=ZERO)
        acc = acc + dotg(jnp.concatenate([w[r, n:n + TWO * LANE, :] for r in range(ND)], axis=ONE), pm, NT)
        cls = KC * me + n + lax.broadcasted_iota(jnp.int32, (TWO * LANE, NIMG), ZERO)
        lg[n:n + TWO * LANE, :] = jnp.where(cls < NCLS, acc, -1e30)
    lab = lab_ref[ZERO:ONE, :].astype(jnp.int32)
    lgv = lg[:]
    hit = KC * me + lax.broadcasted_iota(jnp.int32, (KC, NIMG), ZERO) == lab
    m = jnp.max(lgv, axis=ZERO, keepdims=True)
    st[ZERO:ONE, :] = m
    st[ONE:TWO, :] = jnp.sum(jnp.exp(lgv - m), axis=ZERO, keepdims=True)
    st[TWO:THREE, :] = jnp.sum(jnp.where(hit, lgv, 0.0), axis=ZERO, keepdims=True)
    st[THREE:, :] = jnp.zeros((SUB - THREE, NIMG), F32)
    cs = ag_all(me, st, sta, ss2, rs2)
    sta[me] = st[:]
    wait_all(cs)
    top = sta[ZERO, ZERO:ONE, :]
    for k in range(ONE, ND):
        top = jnp.maximum(top, sta[k, ZERO:ONE, :])
    z = jnp.zeros((ONE, NIMG), F32)
    picked = jnp.zeros((ONE, NIMG), F32)
    for k in range(ND):
        z = z + sta[k, ONE:TWO, :] * jnp.exp(sta[k, ZERO:ONE, :] - top)
        picked = picked + sta[k, TWO:THREE, :]
    logz = top + jnp.log(z)
    loss_ref[:] = jnp.broadcast_to(jnp.sum(logz - picked, axis=ONE, keepdims=True) * (1.0 / NIMG), (SUB, LANE))
    gb_ref[:] = jnp.zeros(gb_ref.shape, F32)
    for q in range(KR):
        n = q * LANE
        hit = KC * me + n + lax.broadcasted_iota(jnp.int32, (LANE, NIMG), ZERO) == lab
        d = (jnp.exp(lg[n:n + LANE, :] - logz) - jnp.where(hit, 1.0, 0.0)) * (1.0 / NIMG)
        dl_ref[n:n + LANE, :] = d.astype(BF)
        gb_ref[q:q + ONE, :] = jnp.sum((d[:, :LANE] + d[:, LANE:]).T, axis=ZERO, keepdims=True)
    for r in range(ZERO, ND, TWO):
        dp = dotg(dl_ref[:], jnp.concatenate([w[r], w[r + ONE]], axis=ONE), TN)
        dps[:, :, r * LANE:(r + TWO) * LANE] = dp.reshape(ND, B, TWO * LANE)
    cs = []
    for d in range(ONE, ND):
        peer = lax.rem(me + d, ND)
        c = rcopy(dps.at[peer], dpr.at[me], ss3.at[d], rs3.at[d], peer)
        c.start()
        cs.append(c)
    dpr[me] = dps[me]
    wait_all(cs)
    acc = dpr[ZERO]
    for k in range(ONE, ND):
        acc = acc + dpr[k]
    dpool_ref[:] = acc


def head(wall, pooled, wp, cid):
    n = (ND,)
    return run(head_kernel, (wall, pooled, wp[7], wp[6]), [HBM] + [VM] * THREE,
        [sds((KC, NIMG), BF), sds((24, LANE), F32), sds((SUB, LANE), F32), sds((B, C), F32), sds((ND, B, C), BF)], [VM] * 5,
        scratch=[pltpu.VMEM((ND, KC, LANE), BF), pltpu.VMEM((KC, NIMG), F32), pltpu.VMEM((B, C), BF), pltpu.VMEM((SUB, NIMG), F32), pltpu.VMEM((ND, SUB, NIMG), F32), pltpu.VMEM((ND, B, C), F32), pltpu.VMEM((ND, B, C), F32)] + [SEM(n)] * 7,
        flops=TWO * TEN**TEN, cid=cid)


def pack_small(dst, dw1_ref, dw2_ref, dbt1_ref, dbt2_ref, dg1_ref, ds1_ref, dg2_ref, ds2_ref, dbc1_ref, dbc2_ref, ws, wl, wh, xs):
    ws[:] = jnp.zeros(ws.shape, F32)
    ws[:, :SP] = dw1_ref[:]
    w1 = ws[:].T
    for j in range(FOUR):
        dst(j, S, FOUR, w1[:S, j * LANE:(j + ONE) * LANE])
    wl[:] = dw2_ref[:, :LANE]
    wh[:, :SP - LANE] = dw2_ref[:, LANE:]
    lane = lax.broadcasted_iota(jnp.int32, (16, LANE), ONE)
    for i in range(49):
        j0 = LANE * i // S
        s0 = LANE * i % S
        lo = wl[pl.ds(j0, 16, stride=32), :]
        hi = wh[pl.ds(j0, 16, stride=32), :]
        if s0 < LANE:
            v = shift_pick(lo, hi, lane, s0)
        else:
            v = pltpu.roll(hi, (TWO * LANE - s0) % LANE, ONE)
        left = S - s0
        if left < LANE:
            nx = wl[pl.ds(j0 + ONE, 16, stride=32), :]
            v = jnp.where(lane < left, v, pltpu.roll(nx, left, ONE))
        dst(HTOK + i, 16, 49, v)
    xs[:] = jnp.zeros(xs.shape, F32)

    def put(r0, v, n):
        for i in range(n):
            xs[r0 + i:r0 + i + ONE, :] = v[:, i * LANE:(i + ONE) * LANE]

    def tot(ref):
        return jnp.sum(ref[:], axis=ZERO, keepdims=True)

    put(ZERO, tot(dg2_ref), SUB)
    put(SUB, tot(ds2_ref), SUB)
    put(16, tot(dbc1_ref), 32)
    put(48, tot(dbc2_ref), SUB)
    x = xs[:]
    r = S - LANE
    lane8 = lax.broadcasted_iota(jnp.int32, (SMR, LANE), ONE)
    xr = pltpu.roll(x, r, ONE)
    xs[:] = jnp.zeros(xs.shape, F32)
    xs[21:77, :] = xr[:56]
    shifted = jnp.where(lane8 >= r, xs[:], 0.0)
    xs[22:78, :] = xr[:56]
    low = jnp.where(lane8 < r, xs[:], 0.0)
    row_i = lax.broadcasted_iota(jnp.int32, (SMR, LANE), ZERO)
    xs[:] = shifted + jnp.where(row_i >= 22, low, 0.0)
    put(ZERO, tot(dg1_ref), SUB)
    put(SUB, tot(ds1_ref), SUB)
    put(16, jnp.sum(dbt1_ref[:].T, axis=ZERO, keepdims=True), FOUR)
    bt2 = jnp.sum(dbt2_ref[:].T, axis=ZERO, keepdims=True)
    xs[20:21, :] = bt2[:, :LANE]
    xs[21:22, :r] = bt2[:, LANE:S]
    dst(TOKR, SMR, ONE, xs[:])
    dst(TOKR + SMR, ND * TP - TOKR - SMR, ONE, jnp.zeros((ND * TP - TOKR - SMR, LANE), F32))


PACK_SCR = [pltpu.VMEM((J, 256), F32), pltpu.VMEM((J, LANE), F32), pltpu.VMEM((J, LANE), F32), pltpu.VMEM((SMR, LANE), F32)]


def pack_kernel(*refs):
    ins = refs[:TEN]
    gb_ref, dgf_ref, dsf_ref, o_ref, ws, wl, wh, xs = refs[TEN:]
    me = lax.axis_index(AX)

    def dst(r0, n, stride, v):
        if stride == ONE:
            o_ref[r0:r0 + n, :] = v
        else:
            o_ref[pl.ds(r0, n, stride=stride), :] = v

    pack_small(dst, *ins, ws, wl, wh, xs)
    base = ND * TP
    o_ref[base:, :] = jnp.zeros((SMF, LANE), F32)
    for r0, ref in ((ZERO, dgf_ref), (SUB, dsf_ref)):
        v = jnp.sum(ref[:], axis=ZERO, keepdims=True)
        for i in range(SUB):
            o_ref[base + r0 + i:base + r0 + i + ONE, :] = v[:, i * LANE:(i + ONE) * LANE]
    o_ref[pl.ds(base + 16 + KR * me, KR), :] = gb_ref[:KR, :]


def pack(parts, gb, dgf, dsf):
    return run(pack_kernel, tuple(parts) + (gb, dgf, dsf), [VM] * 13, sds((ND * TP + SMF, LANE), F32), VM, scratch=PACK_SCR)


def untile(g_ref, o_ref, me, r0=ZERO):
    off = TOKR - STEPR * me + r0

    def go(nj, acc0):
        def step(i, acc):
            for j in range(nj):
                v = g_ref[i * nj + j]
                o_ref[pl.ds(off + i * SUB * nj + j, SUB, stride=nj), :] = v
                acc = acc + v * v
            return acc

        return lax.fori_loop(ZERO, g_ref.shape[ZERO] // nj, step, acc0)

    return go


def fin_kernel(g_ref, tot_ref, sqh_ref, o_ref, sg_ref, sq_ref):
    me = lax.axis_index(AX)
    go = untile(g_ref, o_ref, me)
    base = ND * TP
    sg = tot_ref[pl.ds(pl.multiple_of(base + SMD * me, SUB), SMD), :]
    sg_ref[:] = sg
    tl = tot_ref[:base, :]
    acc = sqh_ref[:] + sum8(sg * sg) + jnp.where(me == ZERO, 1.0, 0.0) * sum8(tl * tl)

    @on(me < ND // TWO)
    def _():
        sq_ref[:] = go(D // LANE, acc)

    @on(me >= ND // TWO)
    def _():
        sq_ref[:] = go(C // LANE, acc)


def fin(g, tot, sqh):
    return run(fin_kernel, (g, tot, sqh), [VM] * THREE, [sds((GROWS, LANE), F32), sds((SMD, LANE), F32), sds((SUB, LANE), F32)], [VM] * THREE)


def finh_kernel(g_ref, sqi_ref, o_ref, sq_ref):
    me = lax.axis_index(AX)
    go = untile(g_ref, o_ref, me, UR // TWO)

    @on(me < ND // TWO)
    def _():
        sq_ref[:] = go(D // LANE, sqi_ref[:])

    @on(me >= ND // TWO)
    def _():
        sq_ref[:] = go(C // LANE, sqi_ref[:])


def finh(g, sqi):
    return run(finh_kernel, (g, sqi), [VM] * TWO, [sds((GROWS, LANE), F32), sds((SUB, LANE), F32)], [VM] * TWO)


def tail_kernel(*refs):
    ins = refs[:TEN]
    g_ref, sqi_ref, gl_ref, o_ref, sca_ref, ws, wl, wh, xs, xb, rb, sb, sqb, sqa, ss, rs, ss2, rs2, ss5, rs5, ss7, rs7 = refs[TEN:]

    def dst(r0, n, stride, v):
        if stride == ONE:
            for q in range(ND):
                a = max(r0, q * TP)
                e = min(r0 + n, (q + ONE) * TP)
                if a < e:
                    xb[a:e, :] = v[a - r0:e - r0]
        else:
            xb[pl.ds(r0, n, stride=stride), :] = v

    pack_small(dst, *ins, ws, wl, wh, xs)
    me = entry_barrier()

    def part(q):
        return xb.at[pl.ds(pl.multiple_of(q * TP, SUB), TP)]

    cs = []
    for d in range(ONE, ND):
        peer = lax.rem(me + d, ND)
        c = rcopy(part(peer), rb.at[me], ss.at[d], rs.at[d], peer)
        c.start()
        cs.append(c)
    rb[me] = xb[pl.ds(pl.multiple_of(me * TP, SUB), TP), :]
    go = untile(g_ref, gl_ref, me)

    @on(me < ND // TWO)
    def _():
        sqb[:] = go(D // LANE, sqi_ref[:])

    @on(me >= ND // TWO)
    def _():
        sqb[:] = go(C // LANE, sqi_ref[:])

    wait_all(cs)
    a = rb[ZERO]
    for k in range(ONE, ND):
        a = a + rb[k]
    sb[:] = a
    sqb[:] += sum8(a * a)
    csq = ag_all(me, sqb, sqa, ss7, rs7)
    sqa[me] = sqb[:]

    def to_first():
        return rcopy(sb, o_ref.at[me], ss2, rs2.at[me], ZERO)

    def to_last():
        return rcopy(sb, o_ref.at[me], ss5, rs5.at[me], ND - ONE)

    @on(me != ZERO)
    def _():
        to_first().start()

    @on(me != ND - ONE)
    def _():
        to_last().start()

    o_ref[me] = sb[:]
    wait_all(csq)
    t = sqa[ZERO]
    for k in range(ONE, ND):
        t = t + sqa[k]
    t = jnp.sum(jnp.sum(t, axis=ZERO, keepdims=True), axis=ONE, keepdims=True)
    sca_ref[:] = jnp.broadcast_to(1.0 / jnp.maximum(1.0, jnp.sqrt(t)), (SUB, LANE))

    @on(me != ZERO)
    def _():
        to_first().wait_send()

    @on(me != ND - ONE)
    def _():
        to_last().wait_send()

    @on(me == ZERO)
    def _():
        for d in range(ONE, ND):
            rcopy(sb, o_ref.at[d], ss2, rs2.at[d], ZERO).wait_recv()

    @on(me == ND - ONE)
    def _():
        for d in range(ND - ONE):
            rcopy(sb, o_ref.at[d], ss5, rs5.at[d], ZERO).wait_recv()


def tail(parts, g, sqi, cid):
    n = (ND,)
    return run(tail_kernel, tuple(parts) + (g, sqi), [VM] * 12,
        [sds((GROWS, LANE), F32), sds((ND, TP, LANE), F32), sds((SUB, LANE), F32)], [VM] * THREE,
        scratch=PACK_SCR + [pltpu.VMEM((ND * TP, LANE), F32), pltpu.VMEM((ND, TP, LANE), F32), pltpu.VMEM((TP, LANE), F32), pltpu.VMEM((SUB, LANE), F32), pltpu.VMEM((ND, SUB, LANE), F32),
            SEM(n), SEM(n), SEM, SEM(n), SEM, SEM(n), SEM(n), SEM(n)], cid=cid)


def adam_math(p, m, v, g, decay):
    m2 = BETA_ONE * m + (1.0 - BETA_ONE) * g
    v2 = BETA_TWO * v + (1.0 - BETA_TWO) * g * g
    mh = m2 * (1.0 / (1.0 - BETA_ONE ** ADAM_STEP))
    vh = v2 * (1.0 / (1.0 - BETA_TWO ** ADAM_STEP))
    return p - LEARN_RATE * (mh / (jnp.sqrt(vh) + ADAM_EPS) + decay * p), m2, v2


HBR = 2816


def head_gsq_kernel(dl_ref, p_ref, sqi_ref, sq_ref):
    @on(pl.program_id(ZERO) == ZERO)
    def _():
        sq_ref[:] = sqi_ref[:]

    g = dot(dl_ref[:], p_ref[:])
    sq_ref[:] += sum8(g * g)


def head_gsq(dl, pc, sq):
    return run(head_gsq_kernel, (dl, pc, sq), [pl.BlockSpec((HBR, NIMG), lambda i: (i, ZERO)), fixed((NIMG, LANE)), fixed((SUB, LANE))],
        sds((SUB, LANE), F32), fixed((SUB, LANE)), grid=ND, flops=TEN**9, nbytes=TEN**7)


ABR = 656
NAB = -(-RSH // ABR)


def head_adam_kernel(sc_ref, dl_ref, pc_ref, p_ref, m_ref, v_ref, po_ref, mo_ref, vo_ref):
    g = dot(dl_ref[:], pc_ref[:]) * sc_ref[ZERO, ZERO]
    po_ref[:], mo_ref[:], vo_ref[:] = adam_math(p_ref[:], m_ref[:], v_ref[:], g, WEIGHT_DECAY)


def head_adam(sc, dl, pc, p, m, v):
    blk = pl.BlockSpec((HAB, LANE), lambda i: (i, ZERO))
    return run(head_adam_kernel, (sc, dl, pc, p, m, v), [SMEM, pl.BlockSpec((HAB, NIMG), lambda i: (i, ZERO)), fixed((NIMG, LANE)), blk, blk, blk],
        [sds(p.shape, F32)] * THREE, [blk] * THREE, grid=-(-NCLS // HAB), flops=TEN**TEN, nbytes=8 * TEN**7)


def layer_adam_kernel(sc_ref, g0_ref, h0_ref, g1_ref, t0_ref, t1_ref, s0_ref, s1_ref, p_ref, m_ref, v_ref, po_ref, mo_ref, vo_ref, gs):
    k = lax.axis_index(AX)
    i = pl.program_id(ZERO)
    off = TOKR - STEPR * k
    sc = sc_ref[ZERO, ZERO]
    lays = ((g0_ref, t0_ref, s0_ref), (g1_ref, t1_ref, s1_ref))
    ri = i * ABR + lax.broadcasted_iota(jnp.int32, (ABR, LANE), ZERO)
    gs[pl.ds(ZERO, ABR, stride=TWO), :] = jnp.where(ri < off + UR // TWO, g0_ref[:], h0_ref[:]) * sc
    gs[pl.ds(ONE, ABR, stride=TWO), :] = g1_ref[:] * sc
    for b in range(THREE):
        @on(i == b)
        def _():
            n = min(ABR, TOKR - b * ABR)
            r = b * ABR + lax.broadcasted_iota(jnp.int32, (n, LANE), ZERO)
            for l in range(TWO):
                g_ref, t_ref, s_ref = lays[l]
                e = min(n, SPR - b * ABR)
                sp = s_ref[b * ABR:b * ABR + e, :]
                if e < n:
                    sp = jnp.concatenate([sp, jnp.zeros((n - e, LANE), F32)], axis=ZERO)
                alt = jnp.where(k == ZERO, t_ref[b * ABR:b * ABR + n, :], sp)
                gs[pl.ds(l, n, stride=TWO), :] = jnp.where(r < off, alt, g_ref[:n, :]) * sc

    @on(jnp.logical_and(i == NAB - ONE, k == ND - ONE))
    def _():
        r0 = RSH - SMR - (NAB - ONE) * ABR
        for l in range(TWO):
            gs[pl.ds(TWO * r0 + l, SMR, stride=TWO), :] = lays[l][ONE][TOKR:TOKR + SMR, :] * sc

    n2 = TWO * ABR
    r2 = TWO * (RSH * k + i * ABR) + lax.broadcasted_iota(jnp.int32, (n2, LANE), ZERO)
    decay = jnp.where(r2 < TWO * MATR, WEIGHT_DECAY, 0.0)
    a, b, c = adam_math(p_ref.reshape(n2, LANE)[:], m_ref.reshape(n2, LANE)[:], v_ref.reshape(n2, LANE)[:], gs[:], decay)
    po_ref.reshape(n2, LANE)[:] = a
    mo_ref.reshape(n2, LANE)[:] = b
    vo_ref.reshape(n2, LANE)[:] = c


def layer_adam(sc, g0, h0, g1, t0, t1, s0, s1, p, m, v):
    blk = pl.BlockSpec((ABR, TWO, LANE), lambda i: (i, ZERO, ZERO))
    gb = pl.BlockSpec((ABR, LANE), lambda i: (i, ZERO))
    return run(layer_adam_kernel, (sc, g0, h0, g1, t0, t1, s0, s1, p, m, v),
        [SMEM, gb, gb, gb] + [fixed(t.shape) for t in (t0, t1, s0, s1)] + [blk] * THREE, [sds(p.shape, F32)] * THREE, [blk] * THREE,
        scratch=[pltpu.VMEM((TWO * ABR, LANE), F32)], grid=NAB, nbytes=6 * TEN**7)


def solution(mesh):
    row_spec = P(AX)
    layer_spec = P(None, AX)
    in_specs = (row_spec, row_spec, layer_spec, row_spec, row_spec, layer_spec, row_spec, row_spec, layer_spec, row_spec, row_spec)
    out_specs = (P(),) + in_specs[TWO:]
    up = [(i, (i + ONE) % ND) for i in range(ND)]

    def scatter(grad, n):
        return lax.psum_scatter(grad.reshape(ND, n, LANE), AX, scatter_dimension=ZERO, tiled=True).reshape(n // SUB, SUB, LANE)

    def device_step(act_in, labels, layer_p, head_w, small_p, layer_m, head_m, small_m, layer_v, head_v, small_v):
        me = lax.axis_index(AX)
        p3 = rows3(layer_p)
        lab = jnp.pad(labels.astype(F32)[None, :], ((ZERO, SUB - ONE), (ZERO, LANE - B)))
        misc = jnp.concatenate([small_p.reshape(SMD, LANE), lab], axis=ZERO)
        t0, t1, tok_all, sm_all, misc_all = start(p3, misc, ONE)
        wg = [lax.all_gather(t, AX, tiled=True) for t in (t0, t1)]
        wp = wprep(tok_all, sm_all, misc_all)
        hidden = act_in
        saved = []
        for l in range(TWO):
            x1, n2, ta, tg = tok_fwd(hidden, wp, l)
            if l == ZERO:
                hw, x1 = lax.optimization_barrier((head_w, x1))
                wall = lax.all_gather(hconv(hw.T), AX)
            x1 = x1.reshape(T, C)
            n2 = n2.reshape(T, C)
            x2, act, gp = ch_fwd(n2, x1, wg[l], wp, l)
            saved.append((hidden, ta, tg, x1, n2, act, gp))
            hidden = x2.reshape(B, SP, C)
        pooled = pool(hidden, wp).reshape(B, C)
        dl, gb, loss, dpool, pall = head(wall, pooled, wp, TWO)
        dl_all = lax.all_gather(dl, AX, tiled=True)
        pc = lax.dynamic_slice_in_dim(pall.reshape(NIMG, C), LANE * me, LANE, axis=ONE)
        d_out, dgf, dsf = lnf_bwd(hidden, dpool.reshape(B // PI, PI, C), wp)
        d_out = d_out.reshape(T, C)
        for l in (ONE, ZERO):
            hid_in, ta, tg, x1, n2, act, gp = saved[l]
            if l:
                dh, dbc1, dbc2 = ch_bwd_a(d_out, gp, wg[l])
                dh, dl_all = lax.optimization_barrier((dh, dl_all))
                grad = dw1_call(n2, dh, dw2_call(act, d_out))
                dh, grad = lax.optimization_barrier((dh, grad))
                shard1 = scatter(grad, UR)
            else:
                g2 = dw2_call(act, d_out, ONE)
                g2, d_out = lax.optimization_barrier((g2, d_out))
                dh, dbc1, dbc2 = ch_bwd_a(d_out, gp, wg[l])
                grad = dw1_call(n2, dh, g2, ONE)
                dh, grad, tot, act = lax.optimization_barrier((dh, grad, tot, act))
                shard_b = scatter(grad, UR // TWO)
                gl1, small_g, sq = fin(shard1, tot, jnp.zeros((SUB, LANE), F32))
                sp1 = lax.ppermute(gl1[RSH:RSH + SPR], AX, up)
                dh, sq, act = lax.optimization_barrier((dh, sq, act))
                grad = dw1_call(n2, dh, dw2_call(act, d_out, ZERO), ZERO)
                dh, grad = lax.optimization_barrier((dh, grad))
                shard_a = scatter(grad, UR // TWO)
            da, dg2, ds2 = ch_bwd_b(dh, wg[l], x1, d_out, wp, l)
            if l == ZERO:
                h0, sq = finh(shard_b, sq)
                sp0 = lax.ppermute(h0[RSH:RSH + SPR], AX, up)
                da, sq = lax.optimization_barrier((da, sq))
            o = tok_bwd(hid_in, da.reshape(B, SP, C), ta, tg, wp, l)
            if l:
                d_out = o[ZERO].reshape(T, C)
                o = o[ONE:]
            parts = tuple(o) + (dg2, ds2, dbc1, dbc2)
            if l:
                sv, d_out = lax.optimization_barrier((pack(parts, gb, dgf, dsf), d_out))
                tot = lax.psum(sv, AX)
        dl_b, first, sp0 = lax.optimization_barrier((dl_all, parts[ZERO], sp0))
        sq = head_gsq(dl_b, pc, sq)
        gl0, tsm, sca = tail((first,) + parts[ONE:], shard_a, sq, FOUR)
        np3, nm3, nv3 = layer_adam(sca, gl0, h0, gl1, tsm.reshape(ND * TP, LANE), tot, sp0, sp1, p3, rows3(layer_m), rows3(layer_v))
        nh, nhm, nhv = head_adam(sca, dl_all, pc, head_w.T, head_m.T, head_v.T)
        nsp, nsm, nsv = adam_math(small_p, small_m, small_v, small_g.reshape(SMD * LANE) * sca[ZERO, ZERO], 0.0)
        return (loss[ZERO, ZERO], unrows3(np3), nh.T, nsp, unrows3(nm3), nhm.T, nsm, unrows3(nv3), nhv.T, nsv)

    return jax.shard_map(device_step, mesh=mesh, in_specs=in_specs, out_specs=out_specs, check_vma=False)
```

```python
import functools
import math
import jax
import jax.numpy as jnp
from jax import lax
from jax.experimental import pallas as pl
from jax.experimental.pallas import tpu as pltpu
from jax.experimental.layout import with_layout_constraint, Layout
from jax.sharding import PartitionSpec as P


F32 = jnp.float32
BF = jnp.bfloat16
LN_EPS = 1e-6
LEARN_RATE = 0.003
BETA_ONE = 0.9
BETA_TWO = 0.999
ADAM_EPS = 1e-8
WEIGHT_DECAY = 0.03
ADAM_STEP = 10
GC0 = math.sqrt(2 / math.pi)
GC1 = GC0 * 0.044715

LANE = 128
SUB = 8
ND = 8
AX = 'fsdp'
B = 32
S = 196
SP = 200
C = 1024
J = 512
D = 4096
NCLS = 21843
NIMG = 256
T = B * SP
KC = 2816
KR = KC // LANE
RSH = 8398
TOKR = 1568
HTOK = TOKR // 2
UNIT = 512
NU = 16
UR = UNIT * NU
STEPR = RSH - UR
SPILL = TOKR - STEPR
SPR = SPILL + 6
MATR = TOKR + ND * UR
SMR = 80
GROWS = RSH + SPILL + SUB
TP = 208
SMF = 192
SMD = SMF // ND
VROW = 16
VLIM = 64 * 1024 * 1024 - 65536
VTAIL = 16 * 1024 * 1024
NT = (((1,), (1,)), ((), ()))
TN = (((0,), (0,)), ((), ()))
VM = pl.BlockSpec(memory_space=pltpu.VMEM)
HBM = pl.BlockSpec(memory_space=pl.ANY)
SMEM = pl.BlockSpec(memory_space=pltpu.SMEM)
SEM = pltpu.SemaphoreType.DMA
VG1, VS1, VG2, VS2, VB2, VB1, VLG, VLS = 0, 1, 2, 3, 4, 5, 9, 10


ZERO, ONE, TWO, THREE, FOUR, TEN = 0, 1, 2, 3, 4, 10


def sds(shape, dt):
    return jax.ShapeDtypeStruct(shape, dt)


def fixed(shape, idx=None, once=False):
    ix = tuple(idx) if idx else (0,) * len(shape)
    return pl.BlockSpec(shape, lambda i: ix, pipeline_mode=pl.Buffered(1) if once else None)


def run(body, ins, in_specs, outs, out_specs, scratch=(), grid=None, flops=10**9, nbytes=10**6, alias={}, cid=None, vlim=VLIM):
    kw = dict(vmem_limit_bytes=vlim)
    if cid is not None:
        kw.update(collective_id=cid, has_side_effects=True)
    if grid:
        kw.update(dimension_semantics=("arbitrary",))
    extra = dict(grid=(grid,)) if grid else {}
    return pl.pallas_call(body, in_specs=in_specs, out_specs=out_specs, out_shape=outs, scratch_shapes=list(scratch),
        input_output_aliases=alias, cost_estimate=pl.CostEstimate(flops=flops, bytes_accessed=nbytes, transcendentals=0),
        compiler_params=pltpu.CompilerParams(**kw), **extra)(*ins)


def on(cond):
    return pl.when(cond)


def unit_stats(xf):
    mean = jnp.sum(xf, axis=-ONE, keepdims=True) * (1.0 / C)
    xc = xf - mean
    rstd = lax.rsqrt(jnp.sum(xc * xc, axis=-ONE, keepdims=True) * (1.0 / C) + LN_EPS)
    return xc * rstd, rstd


def sum8(v):
    return jnp.sum(v.reshape(v.shape[ZERO] // SUB, SUB, v.shape[ONE]), axis=ZERO)


def ln_bwd(nh, rstd, dy, g):
    dxh = dy * g
    m1 = jnp.sum(dxh, axis=-ONE, keepdims=True) * (1.0 / C)
    m2 = jnp.sum(dxh * nh, axis=-ONE, keepdims=True) * (1.0 / C)
    return rstd * (dxh - m1 - nh * m2)


def gelu_both(h):
    u = h * h
    t = jnp.tanh(h * (GC0 + GC1 * u))
    cdf = 0.5 + 0.5 * t
    a = h * cdf
    return a.astype(BF), cdf + (a * (1.0 - t)) * (GC0 + (THREE * GC1) * u)


def wcols(w_ref, c0, n):
    r = w_ref.shape[ZERO] * 16
    return jnp.concatenate([w_ref[:, j].reshape(r, LANE) for j in range(c0 // LANE, (c0 + n) // LANE)], axis=ONE)


def wrows(w_ref, r0, n):
    return jnp.concatenate([w_ref[r0 // 16:(r0 + n) // 16, j].reshape(n, LANE) for j in range(w_ref.shape[ONE])], axis=ONE)


def dot(a, b):
    return jnp.dot(a, b, preferred_element_type=F32)


def dotg(a, b, dn):
    return lax.dot_general(a, b, dn, preferred_element_type=F32)


def entry_barrier():
    me = lax.axis_index(AX)
    b = pltpu.get_barrier_semaphore()
    for d in range(ONE, ND):
        pl.semaphore_signal(b, inc=ONE, device_id=(lax.rem(me + d, ND),), device_id_type=pl.DeviceIdType.MESH)
    pl.semaphore_wait(b, ND - ONE)
    return me


def rcopy(src, dst, ss, rs, dev):
    return pltpu.make_async_remote_copy(src_ref=src, dst_ref=dst, send_sem=ss, recv_sem=rs, device_id=(dev,), device_id_type=pl.DeviceIdType.MESH)


def ag_all(me, src, dst, ss, rs):
    cs = []
    for d in range(ONE, ND):
        c = rcopy(src, dst.at[me], ss.at[d], rs.at[d], lax.rem(me + d, ND))
        c.start()
        cs.append(c)
    return cs


def wait_all(cs):
    for c in cs:
        c.wait()


def rows3(a):
    b = with_layout_constraint(a.reshape(TWO, RSH, LANE), Layout(major_to_minor=(ONE, ZERO, TWO)))
    return b.transpose(ONE, ZERO, TWO)


def unrows3(a):
    b = with_layout_constraint(a.transpose(ONE, ZERO, TWO), Layout(major_to_minor=(ONE, ZERO, TWO)))
    return b.reshape(TWO, RSH * LANE)


OWN = NU - THREE
LEFT = RSH - (TOKR - STEPR * (ND - ONE)) - UNIT * OWN
NTILE = UNIT // 16


def tiles(o_ref, src, r0, step_rows, nj, n, t0):
    def step(i, _):
        for j in range(nj):
            o_ref[t0 + i * nj + j] = src[pl.ds(r0 + (i * 16 * nj + j) * step_rows, 16, stride=nj * step_rows), :].astype(BF)
        return ZERO

    lax.fori_loop(ZERO, n * NTILE // nj, step, ZERO)


def by_half(me, f):
    @on(me < ND // TWO)
    def _():
        f(D // LANE)

    @on(me >= ND // TWO)
    def _():
        f(C // LANE)


TQ = TOKR // ND


def prep_kernel(p_ref, o0_ref, o1_ref, shs0_ref, shs1_ref, toks_ref, tok1_ref, sms_ref, left0_ref, left1_ref):
    me = lax.axis_index(AX)
    src = p_ref.reshape(TWO * RSH, LANE)
    for l in range(TWO):
        (shs0_ref, shs1_ref)[l][:] = src[pl.ds(l, SPR, stride=TWO), :].astype(BF)
        (left0_ref, left1_ref)[l][:] = src[pl.ds(TWO * (RSH - LEFT) + l, LEFT, stride=TWO), :]
        sms_ref[l] = src[pl.ds(TWO * (RSH - SMR) + l, SMR, stride=TWO), :].astype(BF)
    off = TOKR - STEPR * me

    def go(nj):
        for l in range(TWO):
            tiles((o0_ref, o1_ref)[l], src, TWO * off + l, TWO, nj, OWN, ZERO)

    by_half(me, go)

    @on(me == ZERO)
    def _():
        for q in range(ND):
            toks_ref[q] = src[pl.ds(TWO * TQ * q, TQ, stride=TWO), :].astype(BF)
        tok1_ref[:] = src[pl.ds(ONE, TOKR, stride=TWO), :].astype(BF).astype(F32)

    @on(me != ZERO)
    def _():
        toks_ref[:] = jnp.zeros(toks_ref.shape, BF)
        tok1_ref[:] = jnp.zeros(tok1_ref.shape, F32)


def prep(p3):
    tile = sds((NU * NTILE, 16, LANE), BF)
    sh = sds((SPR, LANE), BF)
    left = sds((LEFT, LANE), F32)
    return run(prep_kernel, (p3,), [VM], [tile, tile, sh, sh, sds((ND, TQ, LANE), BF), sds((TOKR, LANE), F32), sds((TWO, SMR, LANE), BF), left, left], [VM] * 9)


def last_units(me, left_ref, shr_ref, z, w):
    z[:LEFT, :] = left_ref[:]
    z[LEFT:, :] = shr_ref[:].astype(F32)
    r0 = LEFT - (RSH - (TOKR - STEPR * me) - UNIT * OWN)
    by_half(me, lambda nj: tiles(w, z, r0, ONE, nj, NU - OWN, ZERO))


def put_last(w, o_ref, sem):
    c = pltpu.make_async_copy(w, o_ref.at[pl.ds(OWN * NTILE, (NU - OWN) * NTILE)], sem)
    c.start()
    return c


LAST_SCR = [pltpu.VMEM((LEFT + SPR, LANE), F32), pltpu.VMEM(((NU - OWN) * NTILE, 16, LANE), BF)]


def fix_kernel(shr_ref, left_ref, u_ref, o_ref, z, w, sem):
    last_units(lax.axis_index(AX), left_ref, shr_ref, z, w)
    put_last(w, o_ref, sem).wait()


def fix(shr, left, t):
    return run(fix_kernel, (shr, left, t), [VM, VM, HBM], sds(t.shape, BF), HBM, scratch=LAST_SCR + [SEM], alias={TWO: ZERO})


def start_kernel(shs, toks, sms, misc_ref, left_ref, u_ref, o_ref, tok_o, sm_o, misc_o, z, w, shr, ss_m, rs_m, ss_s, rs_s, ss_t, rs_t, ss_u, ss_h, rs_h, ss_w):
    me = entry_barrier()
    sh = rcopy(shs, shr, ss_h, rs_h, lax.rem(me + ND - ONE, ND))
    sh.start()

    def first_send(d):
        return rcopy(toks.at[d], tok_o.at[d], ss_t.at[d], rs_t.at[d], d)

    def zero_send(d):
        return rcopy(toks.at[ZERO], tok_o.at[ZERO], ss_u.at[d], rs_t.at[ZERO], d)

    def piece(q, d):
        return rcopy(tok_o.at[q], tok_o.at[q], ss_t.at[d], rs_t.at[q], lax.rem(me - ONE + d, ND - ONE) + ONE)

    def small(d):
        return rcopy(sms, sm_o, ss_s.at[d], rs_s, d)

    @on(me == ZERO)
    def _():
        for d in range(ONE, ND):
            first_send(d).start()
        for d in range(ONE, ND):
            zero_send(d).start()
        tok_o[:] = toks[:]

    @on(me == ND - ONE)
    def _():
        for d in range(ND - ONE):
            small(d).start()
        sm_o[:] = sms[:]

    csm = ag_all(me, misc_ref, misc_o, ss_m, rs_m)
    misc_o[me] = misc_ref[:]

    @on(me > ZERO)
    def _():
        piece(me, ZERO).wait_recv()
        for d in range(ONE, ND - ONE):
            piece(me, d).start()

    sh.wait()
    last_units(me, left_ref, shr, z, w)
    cw = put_last(w, o_ref, ss_w)
    wait_all(csm)

    @on(me < ND - ONE)
    def _():
        small(ZERO).wait_recv()

    @on(me > ZERO)
    def _():
        for d in range(ND - ONE):
            piece(lax.rem(me + ONE + d, ND), ZERO).wait_recv()
        for d in range(ONE, ND - ONE):
            piece(me, d).wait_send()

    @on(me == ZERO)
    def _():
        for d in range(ONE, ND):
            first_send(d).wait_send()
            zero_send(d).wait_send()

    @on(me == ND - ONE)
    def _():
        for d in range(ND - ONE):
            small(d).wait_send()

    cw.wait()


def start(shs, toks, sms, misc, left, t, cid):
    n = (ND,)
    return run(start_kernel, (shs, toks, sms, misc, left, t), [VM] * 5 + [HBM],
        [sds(t.shape, BF), sds(toks.shape, BF), sds(sms.shape, BF), sds(n + misc.shape, F32)], [HBM] + [VM] * THREE,
        scratch=LAST_SCR + [pltpu.VMEM((SPR, LANE), BF), SEM(n), SEM(n), SEM(n), SEM, SEM(n), SEM(n), SEM(n), SEM, SEM, SEM],
        alias={5: ZERO}, flops=TEN**TEN, cid=cid)


def shift_pick(a, b, lane, r):
    return jnp.where(lane < LANE - r, pltpu.roll(a, (LANE - r) % LANE, ONE), pltpu.roll(b, (LANE - r) % LANE, ONE))


def wprep_kernel(l, tok_ref, sm_ref, misc_ref, w1a_ref, w1t_ref, w2p_ref, w2t_ref, b2c_ref, vec_ref, *rest):
    tf, w1s, w2l, w2h, sf, sg = rest[-6:]
    me = lax.axis_index(AX)
    for k in range(ND):
        sf[k * SMD:(k + ONE) * SMD, :] = misc_ref[k, :SMD, :].astype(BF).astype(F32)
    if l == ZERO:
        lab_ref, bias_ref = rest[:TWO]
        for k in range(ND):
            lab_ref[:, k * B:(k + ONE) * B] = jnp.broadcast_to(misc_ref[k, SMD:SMD + ONE, :B], (SUB, B))
            tf[k * TQ:(k + ONE) * TQ, :] = tok_ref[k].astype(F32)
        bias_ref[:] = jnp.zeros(bias_ref.shape, F32)
        bias_ref[:KR, :] = sf[pl.ds(16 + KR * me, KR), :]
    else:
        tf[:TOKR, :] = tok_ref[:]
    vec_ref[:] = jnp.zeros(vec_ref.shape, F32)
    w1s[:] = jnp.zeros(w1s.shape, F32)
    lane = lax.broadcasted_iota(jnp.int32, (16, LANE), ONE)

    def put(row, src, r0, n):
        for i in range(n):
            vec_ref[ZERO, row + i // SUB:row + i // SUB + ONE, (i % SUB) * LANE:(i % SUB + ONE) * LANE] = src[r0 + i:r0 + i + ONE, :]

    smf = sm_ref[l].astype(F32)
    sg[:SMR, :] = smf
    for j in range(FOUR):
        w1s[:S, j * LANE:(j + ONE) * LANE] = tf[pl.ds(j, S, stride=FOUR), :]
        w1s[S:S + ONE, j * LANE:(j + ONE) * LANE] = sg[16 + j:17 + j, :]
    for b in range(32):
        p = S * b
        r0 = HTOK + p // LANE
        o = p % LANE
        x = [tf[pl.ds(r0 + q, 16, stride=49), :] for q in range(THREE if o + S > TWO * LANE else TWO)]
        w2l[pl.ds(b, 16, stride=32), :] = shift_pick(x[ZERO], x[ONE], lane, o)
        hi = shift_pick(x[ONE], x[-ONE], lane, o)
        w2h[pl.ds(b, 16, stride=32), :] = jnp.where(lane < S - LANE, hi, 0.0)
    w1 = w1s[:]
    w2 = jnp.concatenate([w2l[:], w2h[:]], axis=ONE)
    w1a_ref[ZERO] = w1[:SP].astype(BF)
    w1t_ref[ZERO] = w1.T[:, :SP].astype(BF)
    w2p_ref[ZERO] = w2[:, :SP].astype(BF)
    w2t_ref[ZERO] = w2.T[:SP].astype(BF)
    put(VG1, sg, ZERO, SUB)
    put(VS1, sg, SUB, SUB)
    b2 = jnp.concatenate([sg[20:21, :], sg[21:22, :]], axis=ONE)
    b2 = jnp.broadcast_to(b2, (SUB, TWO * LANE)).T[:SP, :ONE]
    rowi = lax.broadcasted_iota(jnp.int32, (SP, LANE), ZERO)
    b2c_ref[ZERO] = jnp.where(rowi < S, jnp.broadcast_to(b2, (SP, LANE)), 0.0)
    lane7 = lax.broadcasted_iota(jnp.int32, (56, LANE), ONE)
    sg[:56, :] = shift_pick(smf[21:77], smf[22:78], lane7, S - LANE)
    put(VG2, sg, ZERO, SUB)
    put(VS2, sg, SUB, SUB)
    put(VB1, sg, 16, 32)
    put(VB2, sg, 48, SUB)
    put(VLG, sf, ZERO, SUB)
    put(VLS, sf, SUB, SUB)


def wprep(l, tok, sm, misc):
    extra = [] if l else [sds((SUB, NIMG), F32), sds((24, LANE), F32)]
    outs = [sds((ONE, SP, J), BF), sds((ONE, J, SP), BF), sds((ONE, J, SP), BF), sds((ONE, SP, J), BF), sds((ONE, SP, LANE), F32), sds((ONE, VROW, C), F32)] + extra
    return run(functools.partial(wprep_kernel, l), (tok, sm, misc), [VM] * THREE, outs, [VM] * len(outs),
        scratch=[pltpu.VMEM((TOKR + SUB, LANE), F32), pltpu.VMEM((256, J), F32), pltpu.VMEM((J, LANE), F32), pltpu.VMEM((J, LANE), F32), pltpu.VMEM((SMF, LANE), F32), pltpu.VMEM((SMR, LANE), F32)],
        flops=5 * TEN**9)


def vec_spec():
    return fixed((ONE, VROW, C))


def lay(shape):
    return fixed((ONE,) + shape)


CW = 256


def tok_fwd_kernel(x_ref, w1t_ref, w2t_ref, b2_ref, v_ref, out_ref, n2_ref, act_ref, gp_ref, n_s):
    @on(pl.program_id(ZERO) == ZERO)
    def _():
        r = lax.broadcasted_iota(jnp.int32, (SP, C), ZERO)
        for im in range(TWO):
            n_s[im] = jnp.where(r == S, 1.0, 0.0).astype(BF)

    for im in range(TWO):
        xf = x_ref[im, :S, :].astype(F32)
        nh, _ = unit_stats(xf)
        n_s[im, :S, :] = (nh * v_ref[ZERO, VG1:VG1 + ONE, :] + v_ref[ZERO, VS1:VS1 + ONE, :]).astype(BF)
    for im in range(TWO):
        cols = []
        for c in range(ZERO, C, CW):
            cs = slice(c, c + CW)
            a, gp = gelu_both(dot(w1t_ref[ZERO], n_s[im, :, cs]))
            act_ref[im, :, cs] = a
            gp_ref[im, :, cs] = gp
            o = dot(w2t_ref[ZERO], a) + b2_ref[ZERO, :, :ONE]
            cols.append((x_ref[im, :S, cs].astype(F32) + o[:S]).astype(BF))
        x1 = jnp.concatenate(cols, axis=ONE)
        out_ref[im, :S, :] = x1
        nh2, _ = unit_stats(x1.astype(F32))
        n2_ref[im, :S, :] = (nh2 * v_ref[ZERO, VG2:VG2 + ONE, :] + v_ref[ZERO, VS2:VS2 + ONE, :]).astype(BF)
        out_ref[im, S:, :] = jnp.zeros((SP - S, C), BF)
        n2_ref[im, S:, :] = jnp.zeros((SP - S, C), BF)


def img(r, n=C):
    return pl.BlockSpec((TWO, r, n), lambda i: (i, ZERO, ZERO))


def tok_fwd(x, wp):
    return run(tok_fwd_kernel, (x, wp[ONE], wp[THREE], wp[FOUR], wp[5]),
        [img(x.shape[ONE]), lay((J, SP)), lay((SP, J)), lay((SP, LANE)), vec_spec()],
        [sds((B, SP, C), BF)] * TWO + [sds((B, J, C), BF), sds((B, J, C), F32)], [img(SP)] * TWO + [img(J)] * TWO,
        scratch=[pltpu.VMEM((TWO, SP, C), BF)], grid=B // TWO, flops=60 * TEN**9, nbytes=14 * TEN**7)


def tok_bwd_kernel(need_dx, x_ref, da_ref, act_ref, gp_ref, w1a_ref, w2p_ref, v_ref, *rest):
    if need_dx:
        dx_ref = rest[ZERO]
        rest = rest[ONE:]
    dw1_ref, dw2_ref, db1_ref, db2_ref, dg_ref, ds_ref, n_s, nh_s, dh_s, dn_s = rest

    @on(pl.program_id(ZERO) == ZERO)
    def _():
        for r in (dw1_ref, dw2_ref, db1_ref, db2_ref, dg_ref, ds_ref, n_s):
            r[:] = jnp.zeros(r.shape, r.dtype)

    rs = []
    for im in range(TWO):
        nh, rstd = unit_stats(x_ref[im, :S, :].astype(F32))
        nh_s[im, :S, :] = nh
        rs.append(rstd)
        n_s[:S, im * C:(im + ONE) * C] = (nh * v_ref[ZERO, VG1:VG1 + ONE, :] + v_ref[ZERO, VS1:VS1 + ONE, :]).astype(BF)
    db1 = db1_ref[:]
    for im in range(TWO):
        for c in range(ZERO, C, CW):
            cs = slice(c, c + CW)
            dact = dot(w2p_ref[ZERO], da_ref[im, :, cs]).astype(BF).astype(F32)
            dh = dact * gp_ref[im, :, cs]
            for k in range(ZERO, CW, LANE):
                db1 = db1 + dh[:, k:k + LANE]
            dhb = dh.astype(BF)
            dh_s[:, im * C + c:im * C + c + CW] = dhb
            dn_s[im, :, cs] = dot(w1a_ref[ZERO], dhb)
    db1_ref[:] = db1
    act2 = jnp.concatenate([act_ref[ZERO], act_ref[ONE]], axis=ONE)
    da2 = jnp.concatenate([da_ref[ZERO], da_ref[ONE]], axis=ONE)
    dw2_ref[:] += dotg(act2, da2, NT)
    dw1_ref[:] += dotg(dh_s[:], n_s[:], NT)
    db2 = db2_ref[:]
    s8 = S // SUB * SUB
    for im in range(TWO):
        for k in range(ZERO, C, LANE):
            db2 = db2 + da_ref[im, :, k:k + LANE].astype(F32)
        dn = dn_s[im, :S, :].astype(BF).astype(F32)
        nh = nh_s[im, :S, :]
        pr = dn * nh
        dg_ref[:] += sum8(pr[:s8])
        ds_ref[:] += sum8(dn[:s8])
        dg_ref[:S - s8] += pr[s8:]
        ds_ref[:S - s8] += dn[s8:]
        if need_dx:
            dx = ln_bwd(nh, rs[im], dn, v_ref[ZERO, VG1:VG1 + ONE, :])
            dx_ref[im, :S, :] = (da_ref[im, :S, :].astype(F32) + dx).astype(BF)
            dx_ref[im, S:, :] = jnp.zeros((SP - S, C), BF)
    db2_ref[:] = db2


def tok_bwd(x, da, act, gp, wp, l):
    acc = [(J, SP), (J, SP), (J, LANE), (SP, LANE), (SUB, C), (SUB, C)]
    dx = [sds((B, SP, C), BF)] if l else []
    return run(functools.partial(tok_bwd_kernel, bool(l)), (x, da, act, gp, wp[ZERO], wp[TWO], wp[5]),
        [img(x.shape[ONE]), img(SP), img(J), img(J), lay((SP, J)), lay((J, SP)), vec_spec()],
        dx + [sds(s, F32) for s in acc], [img(SP)] * len(dx) + [fixed(s) for s in acc],
        scratch=[pltpu.VMEM((SP, TWO * C), BF), pltpu.VMEM((TWO, SP, C), F32), pltpu.VMEM((J, TWO * C), BF), pltpu.VMEM((TWO, SP, C), F32)],
        grid=B // TWO, flops=60 * TEN**9, nbytes=14 * TEN**7)


M = 400
DC = 512


def row(n):
    return pl.BlockSpec((M, n), lambda i: (i, ZERO))


def wspec(h):
    return fixed((64, 32, 16, LANE) if h == ZERO else (256, SUB, 16, LANE), (h, ZERO, ZERO, ZERO), True)


def pair(n):
    return pl.BlockSpec((ONE, TWO, n), lambda i: (i, ZERO, ZERO))


def ch_fwd_kernel(n2_ref, x1_ref, w1_ref, w2_ref, v_ref, x2_ref, act_ref, gp_ref, *pool_ref):
    n2 = n2_ref[:]
    for k in range(D // DC):
        ks = slice(k * DC, (k + ONE) * DC)
        r = VB1 + k // TWO
        b = v_ref[ZERO, r:r + ONE, (k % TWO) * DC:(k % TWO + ONE) * DC]
        act_ref[:, ks], gp_ref[:, ks] = gelu_both(dot(n2, wcols(w1_ref, k * DC, DC)) + b)
    for c in range(ZERO, C, CW):
        cs = slice(c, c + CW)
        o = dot(act_ref[:], wcols(w2_ref, c, CW)) + v_ref[ZERO, VB2:VB2 + ONE, cs]
        x2_ref[:, cs] = (x1_ref[:, cs].astype(F32) + o).astype(BF)
    if pool_ref:
        nh, _ = unit_stats(x2_ref[:].astype(F32))
        n = (nh * v_ref[ZERO, VLG:VLG + ONE, :] + v_ref[ZERO, VLS:VLS + ONE, :]).astype(BF).astype(F32)
        for im in range(TWO):
            pool_ref[ZERO][ZERO, im:im + ONE, :] = jnp.sum(n[im * SP:im * SP + S], axis=ZERO, keepdims=True) * (1.0 / S)


def w_views(wg):
    return wg.reshape(128, 32, 16, LANE), wg.reshape(512, SUB, 16, LANE)


def ch_fwd(n2, x1, wg, wp, l):
    return run(ch_fwd_kernel, (n2, x1) + w_views(wg) + (wp[5],), [row(C), row(C), wspec(ZERO), wspec(ONE), vec_spec()],
        [sds((T, C), BF), sds((T, D), BF), sds((T, D), F32)] + [sds((B // TWO, TWO, C), F32)] * l, [row(C), row(D), row(D)] + [pair(C)] * l,
        grid=T // M, flops=FOUR * T * C * D, nbytes=T * D * 6)


def ch_bwd_a_kernel(do_ref, gp_ref, w2_ref, dh_ref, db1_ref, db2_ref):
    @on(pl.program_id(ZERO) == ZERO)
    def _():
        db1_ref[:] = jnp.zeros(db1_ref.shape, F32)
        db2_ref[:] = jnp.zeros(db2_ref.shape, F32)

    do = do_ref[:]
    db2_ref[:] += sum8(do.astype(F32))
    for k in range(D // DC):
        ks = slice(k * DC, (k + ONE) * DC)
        da = dotg(do, wrows(w2_ref, k * DC, DC), NT).astype(BF).astype(F32)
        dh = da * gp_ref[:, ks]
        db1_ref[:, ks] += sum8(dh)
        dh_ref[:, ks] = dh.astype(BF)


def ch_bwd_top_kernel(x2_ref, dp_ref, v_ref, gp_ref, w2_ref, dh_ref, db1_ref, db2_ref, do_ref, dg_ref, ds_ref):
    @on(pl.program_id(ZERO) == ZERO)
    def _():
        dg_ref[:] = jnp.zeros(dg_ref.shape, F32)
        ds_ref[:] = jnp.zeros(ds_ref.shape, F32)

    g = v_ref[ZERO, VLG:VLG + ONE, :]
    r = lax.broadcasted_iota(jnp.int32, (SP, ONE), ZERO)
    xf = x2_ref[:].astype(F32)
    out = []
    for im in range(TWO):
        dn = (dp_ref[ZERO, im:im + ONE, :] * (1.0 / S)).astype(BF).astype(F32)
        nh, rstd = unit_stats(xf[im * SP:(im + ONE) * SP])
        dxh = dn * g
        m1 = jnp.sum(dxh, axis=-ONE, keepdims=True) * (1.0 / C)
        m2 = jnp.sum(dxh * nh, axis=-ONE, keepdims=True) * (1.0 / C)
        out.append(jnp.where(r < S, rstd * ((dxh - m1) - nh * m2), 0.0))
        dg_ref[ZERO:ONE, :] += dn * jnp.sum(nh[:S], axis=ZERO, keepdims=True)
        ds_ref[ZERO:ONE, :] += dn * float(S)
    do_ref[:] = jnp.concatenate(out, axis=ZERO).astype(BF)
    ch_bwd_a_kernel(do_ref, gp_ref, w2_ref, dh_ref, db1_ref, db2_ref)


def ch_bwd_a(do, gp, wg):
    return run(ch_bwd_a_kernel, (do, gp, w_views(wg)[ONE]), [row(C), row(D), wspec(ONE)],
        [sds((T, D), BF), sds((SUB, D), F32), sds((SUB, C), F32)], [row(D), fixed((SUB, D)), fixed((SUB, C))],
        grid=T // M, flops=TWO * T * C * D, nbytes=T * D * 6)


def ch_bwd_top(x2, dp, gp, wg, wp):
    return run(ch_bwd_top_kernel, (x2, dp, wp[5], gp, w_views(wg)[ONE]), [row(C), pair(C), vec_spec(), row(D), wspec(ONE)],
        [sds((T, D), BF), sds((SUB, D), F32), sds((SUB, C), F32), sds((T, C), BF), sds((SUB, C), F32), sds((SUB, C), F32)],
        [row(D), fixed((SUB, D)), fixed((SUB, C)), row(C), fixed((SUB, C)), fixed((SUB, C))],
        grid=T // M, flops=TWO * T * C * D, nbytes=T * D * 6)


def ch_bwd_b_kernel(dh_ref, w1_ref, x1_ref, do_ref, v_ref, da_ref, dg_ref, ds_ref, dn_s):
    @on(pl.program_id(ZERO) == ZERO)
    def _():
        dg_ref[:] = jnp.zeros(dg_ref.shape, F32)
        ds_ref[:] = jnp.zeros(ds_ref.shape, F32)

    for c in range(ZERO, C, CW):
        dn_s[:, c:c + CW] = dotg(dh_ref[:], wrows(w1_ref, c, CW), NT)
    dy = dn_s[:].astype(BF).astype(F32)
    nh, rstd = unit_stats(x1_ref[:].astype(F32))
    dx = ln_bwd(nh, rstd, dy, v_ref[ZERO, VG2:VG2 + ONE, :])
    dg_ref[:] += sum8(dy * nh)
    ds_ref[:] += sum8(dy)
    r = lax.rem(lax.broadcasted_iota(jnp.int32, (M, ONE), ZERO), SP)
    da_ref[:] = jnp.where(r < S, do_ref[:].astype(F32) + dx, 0.0).astype(BF)


def ch_bwd_b(dh, wg, x1, do, wp):
    return run(ch_bwd_b_kernel, (dh, w_views(wg)[ZERO], x1, do, wp[5]), [row(D), wspec(ZERO), row(C), row(C), vec_spec()],
        [sds((T, C), BF)] + [sds((SUB, C), F32)] * TWO, [row(C)] + [fixed((SUB, C))] * TWO,
        scratch=[pltpu.VMEM((M, C), F32)], grid=T // M, flops=TWO * T * C * D, nbytes=T * D * THREE)


def dw2_kernel(a_ref, b_ref, o_ref):
    r = dotg(a_ref[:], b_ref[:], TN)
    for j in range(C // LANE):
        o_ref[ZERO, :, j] = r[:, LANE * j:LANE * (j + ONE)].reshape(DC // SUB, SUB, LANE)


def dw2_call(act, do, h=None):
    q = C // DC
    own = ND // TWO
    full = h is None
    a_spec = pl.BlockSpec((T, DC), (lambda i: (ZERO, i)) if full else (lambda i: (ZERO, q * i + h)))
    o_map = (lambda i: (own + i // q, lax.rem(i, q), ZERO, ZERO, ZERO)) if full else (lambda i: (own + i, ZERO, ZERO, ZERO, ZERO))
    n = C if full else DC
    return run(dw2_kernel, (act, do), [a_spec, fixed((T, C), once=True)],
        sds((ND, n // SUB, SUB, SUB, LANE), F32), pl.BlockSpec((ONE, DC // SUB, SUB, SUB, LANE), o_map),
        grid=D // DC * n // C, flops=TWO * T * n * D, nbytes=T * D * THREE)


def dw1_kernel(*refs):
    a = jnp.concatenate([r[:] for r in refs[:-THREE]], axis=ONE)
    b_ref, _, o_ref = refs[-THREE:]
    r = dotg(a, b_ref[:], TN)
    for j in range(DC // LANE):
        o_ref[:, :, j] = r[:, LANE * j:LANE * (j + ONE)].reshape(o_ref.shape[:TWO] + (SUB, LANE))


def col_spec(k):
    return fixed((T, LANE), (ZERO, k), True)


def dw1_call(n2, dh, g, h=None):
    full = h is None
    own = ND // TWO
    specs = [fixed((T, C), once=True)] if full else [col_spec(TWO * k + h) for k in range(own)]
    rb = 32 if full else 16
    na = len(specs)
    shape = (ND, rb, 32, SUB, LANE)
    return run(dw1_kernel, (n2,) * na + (dh, g.reshape(shape)), specs + [pl.BlockSpec((T, DC), lambda i: (ZERO, i)), HBM],
        sds(shape, F32), pl.BlockSpec((own, rb, DC // LANE, SUB, LANE), lambda i: (ZERO, ZERO, i, ZERO, ZERO)), alias={na + ONE: ZERO},
        grid=D // DC, flops=TWO * T * (rb * 32) * D, nbytes=T * D * THREE)


HAB = 5632
HAA = 5632


def hconv_kernel(w_ref, o_ref):
    r = pl.program_id(ZERO) * HAB + lax.broadcasted_iota(jnp.int32, (HAB, LANE), ZERO)
    o_ref[:] = jnp.where(r < NCLS, w_ref[:], 0.0).astype(BF)


def hconv(wt):
    blk = pl.BlockSpec((HAB, LANE), lambda i: (i, ZERO))
    return run(hconv_kernel, (wt,), [blk], sds((ND * KC, LANE), BF), blk, grid=ND * KC // HAB, nbytes=TWO * TEN**7)


def head_kernel(*refs):
    wall_ref, pooled_ref, bias_ref, lab_ref, dl_ref, gb_ref, loss_ref, dpool_ref, pall_ref, sqh_ref, w, lg, pb, st, sta, dps, dpr, ws, ss, rs, ss2, rs2, ss3, rs3 = refs
    for i in range(B // TWO):
        pb[TWO * i:TWO * i + TWO, :] = pooled_ref[i].astype(BF)
    row0 = pl.multiple_of(KC * lax.axis_index(AX), KC)
    cw = [pltpu.make_async_copy(wall_ref.at[r, pl.ds(row0, KC)], w.at[r], ws.at[r]) for r in range(ND)]
    for c in cw:
        c.start()
    me = entry_barrier()
    cs = ag_all(me, pb, pall_ref, ss, rs)
    pall_ref[me] = pb[:]
    wait_all(cs)

    wait_all(cw)
    bt = bias_ref[:].T
    pm = pall_ref[:].reshape(NIMG, C)
    for q in range(KR // TWO):
        n = q * TWO * LANE
        acc = jnp.concatenate([jnp.broadcast_to(bt[:, TWO * q + k:TWO * q + k + ONE], (LANE, NIMG)) for k in range(TWO)], axis=ZERO)
        acc = acc + dotg(jnp.concatenate([w[r, n:n + TWO * LANE, :] for r in range(ND)], axis=ONE), pm, NT)
        cls = KC * me + n + lax.broadcasted_iota(jnp.int32, (TWO * LANE, NIMG), ZERO)
        lg[n:n + TWO * LANE, :] = jnp.where(cls < NCLS, acc, -1e30)
    lab = lab_ref[ZERO:ONE, :].astype(jnp.int32)
    lgv = lg[:]
    hit = KC * me + lax.broadcasted_iota(jnp.int32, (KC, NIMG), ZERO) == lab
    m = jnp.max(lgv, axis=ZERO, keepdims=True)
    st[ZERO:ONE, :] = m
    st[ONE:TWO, :] = jnp.sum(jnp.exp(lgv - m), axis=ZERO, keepdims=True)
    st[TWO:THREE, :] = jnp.sum(jnp.where(hit, lgv, 0.0), axis=ZERO, keepdims=True)
    st[THREE:, :] = jnp.zeros((SUB - THREE, NIMG), F32)
    cs = ag_all(me, st, sta, ss2, rs2)
    sta[me] = st[:]
    wait_all(cs)
    top = sta[ZERO, ZERO:ONE, :]
    for k in range(ONE, ND):
        top = jnp.maximum(top, sta[k, ZERO:ONE, :])
    z = jnp.zeros((ONE, NIMG), F32)
    picked = jnp.zeros((ONE, NIMG), F32)
    for k in range(ND):
        z = z + sta[k, ONE:TWO, :] * jnp.exp(sta[k, ZERO:ONE, :] - top)
        picked = picked + sta[k, TWO:THREE, :]
    logz = top + jnp.log(z)
    loss_ref[:] = jnp.broadcast_to(jnp.sum(logz - picked, axis=ONE, keepdims=True) * (1.0 / NIMG), (SUB, LANE))
    gb_ref[:] = jnp.zeros(gb_ref.shape, F32)
    for q in range(KR):
        n = q * LANE
        hit = KC * me + n + lax.broadcasted_iota(jnp.int32, (LANE, NIMG), ZERO) == lab
        d = (jnp.exp(lg[n:n + LANE, :] - logz) - jnp.where(hit, 1.0, 0.0)) * (1.0 / NIMG)
        dl_ref[n:n + LANE, :] = d.astype(BF)
        gb_ref[q:q + ONE, :] = jnp.sum((d[:, :LANE] + d[:, LANE:]).T, axis=ZERO, keepdims=True)
    for r in range(ZERO, ND, TWO):
        dp = dotg(dl_ref[:], jnp.concatenate([w[r], w[r + ONE]], axis=ONE), TN)
        dps[:, :, r * LANE:(r + TWO) * LANE] = dp.reshape(ND, B, TWO * LANE)
    cs = []
    for d in range(ONE, ND):
        peer = lax.rem(me + d, ND)
        c = rcopy(dps.at[peer], dpr.at[me], ss3.at[d], rs3.at[d], peer)
        c.start()
        cs.append(c)
    dpr[me] = dps[me]
    gram = dotg(pm, pm, NT) * dotg(dl_ref[:], dl_ref[:], TN)
    sqh_ref[:] = sum8(gram[:, :LANE] + gram[:, LANE:])
    wait_all(cs)
    acc = dpr[ZERO]
    for k in range(ONE, ND):
        acc = acc + dpr[k]
    for i in range(B // TWO):
        dpool_ref[i] = acc[TWO * i:TWO * i + TWO]


def head(wall, pooled, wp, cid):
    n = (ND,)
    return run(head_kernel, (wall, pooled, wp[7], wp[6]), [HBM] + [VM] * THREE,
        [sds((KC, NIMG), BF), sds((24, LANE), F32), sds((SUB, LANE), F32), sds((B // TWO, TWO, C), F32), sds((ND, B, C), BF), sds((SUB, LANE), F32)], [VM] * 6,
        scratch=[pltpu.VMEM((ND, KC, LANE), BF), pltpu.VMEM((KC, NIMG), F32), pltpu.VMEM((B, C), BF), pltpu.VMEM((SUB, NIMG), F32), pltpu.VMEM((ND, SUB, NIMG), F32), pltpu.VMEM((ND, B, C), F32), pltpu.VMEM((ND, B, C), F32)] + [SEM(n)] * 7,
        flops=TWO * TEN**TEN, cid=cid)


def pack_small(dst, dw1_ref, dw2_ref, dbt1_ref, dbt2_ref, dg1_ref, ds1_ref, dg2_ref, ds2_ref, dbc1_ref, dbc2_ref, ws, wl, wh, xs):
    ws[:] = jnp.zeros(ws.shape, F32)
    ws[:, :SP] = dw1_ref[:]
    w1 = ws[:].T
    for j in range(FOUR):
        dst(j, S, FOUR, w1[:S, j * LANE:(j + ONE) * LANE])
    wl[:] = dw2_ref[:, :LANE]
    wh[:, :SP - LANE] = dw2_ref[:, LANE:]
    lane = lax.broadcasted_iota(jnp.int32, (16, LANE), ONE)
    for i in range(49):
        j0 = LANE * i // S
        s0 = LANE * i % S
        lo = wl[pl.ds(j0, 16, stride=32), :]
        hi = wh[pl.ds(j0, 16, stride=32), :]
        if s0 < LANE:
            v = shift_pick(lo, hi, lane, s0)
        else:
            v = pltpu.roll(hi, (TWO * LANE - s0) % LANE, ONE)
        left = S - s0
        if left < LANE:
            nx = wl[pl.ds(j0 + ONE, 16, stride=32), :]
            v = jnp.where(lane < left, v, pltpu.roll(nx, left, ONE))
        dst(HTOK + i, 16, 49, v)
    xs[:] = jnp.zeros(xs.shape, F32)

    def put(r0, v, n):
        for i in range(n):
            xs[r0 + i:r0 + i + ONE, :] = v[:, i * LANE:(i + ONE) * LANE]

    def tot(ref):
        return jnp.sum(ref[:], axis=ZERO, keepdims=True)

    put(ZERO, tot(dg2_ref), SUB)
    put(SUB, tot(ds2_ref), SUB)
    put(16, tot(dbc1_ref), 32)
    put(48, tot(dbc2_ref), SUB)
    x = xs[:]
    r = S - LANE
    lane8 = lax.broadcasted_iota(jnp.int32, (SMR, LANE), ONE)
    xr = pltpu.roll(x, r, ONE)
    xs[:] = jnp.zeros(xs.shape, F32)
    xs[21:77, :] = xr[:56]
    shifted = jnp.where(lane8 >= r, xs[:], 0.0)
    xs[22:78, :] = xr[:56]
    low = jnp.where(lane8 < r, xs[:], 0.0)
    row_i = lax.broadcasted_iota(jnp.int32, (SMR, LANE), ZERO)
    xs[:] = shifted + jnp.where(row_i >= 22, low, 0.0)
    put(ZERO, tot(dg1_ref), SUB)
    put(SUB, tot(ds1_ref), SUB)
    put(16, jnp.sum(dbt1_ref[:].T, axis=ZERO, keepdims=True), FOUR)
    bt2 = jnp.sum(dbt2_ref[:].T, axis=ZERO, keepdims=True)
    xs[20:21, :] = bt2[:, :LANE]
    xs[21:22, :r] = bt2[:, LANE:S]
    dst(TOKR, SMR, ONE, xs[:])
    dst(TOKR + SMR, ND * TP - TOKR - SMR, ONE, jnp.zeros((ND * TP - TOKR - SMR, LANE), F32))


PACK_SCR = [pltpu.VMEM((J, 256), F32), pltpu.VMEM((J, LANE), F32), pltpu.VMEM((J, LANE), F32), pltpu.VMEM((SMR, LANE), F32)]


def pack_kernel(extra, *refs):
    ins = refs[:TEN]
    o_ref, ws, wl, wh, xs = refs[-5:]

    def dst(r0, n, stride, v):
        if stride == ONE:
            o_ref[r0:r0 + n, :] = v
        else:
            o_ref[pl.ds(r0, n, stride=stride), :] = v

    pack_small(dst, *ins, ws, wl, wh, xs)
    if not extra:
        return
    gb_ref, dgf_ref, dsf_ref = refs[TEN:13]
    me = lax.axis_index(AX)
    base = ND * TP
    o_ref[base:, :] = jnp.zeros((SMF, LANE), F32)
    for r0, ref in ((ZERO, dgf_ref), (SUB, dsf_ref)):
        v = jnp.sum(ref[:], axis=ZERO, keepdims=True)
        for i in range(SUB):
            o_ref[base + r0 + i:base + r0 + i + ONE, :] = v[:, i * LANE:(i + ONE) * LANE]
    o_ref[pl.ds(base + 16 + KR * me, KR), :] = gb_ref[:KR, :]


def pack(parts, extra=()):
    ins = tuple(parts) + extra
    rows = ND * TP + (SMF if extra else ZERO)
    return run(functools.partial(pack_kernel, bool(extra)), ins, [VM] * len(ins), sds((rows, LANE), F32), VM, scratch=PACK_SCR)


def untile(g_ref, o_ref, me, r0=ZERO):
    off = TOKR - STEPR * me + r0

    def go(nj, acc0):
        def step(i, acc):
            for j in range(nj):
                v = g_ref[i * nj + j]
                o_ref[pl.ds(off + i * SUB * nj + j, SUB, stride=nj), :] = v
                acc = acc + v * v
            return acc

        return lax.fori_loop(ZERO, g_ref.shape[ZERO] // nj, step, acc0)

    return go


def fin_kernel(g_ref, tot_ref, sqh_ref, o_ref, sg_ref, sq_ref, sp_ref):
    me = lax.axis_index(AX)
    go = untile(g_ref, o_ref, me)
    base = ND * TP
    sg = tot_ref[pl.ds(pl.multiple_of(base + SMD * me, SUB), SMD), :]
    sg_ref[:] = sg
    tl = tot_ref[:base, :]
    acc = sqh_ref[:] + sum8(sg * sg) + jnp.where(me == ZERO, 1.0, 0.0) * sum8(tl * tl)

    @on(me < ND // TWO)
    def _():
        sq_ref[:] = go(D // LANE, acc)

    @on(me >= ND // TWO)
    def _():
        sq_ref[:] = go(C // LANE, acc)

    sp_ref[:] = o_ref[RSH:RSH + SPR, :]


def fin(g, tot, sqh):
    return run(fin_kernel, (g, tot, sqh), [VM] * THREE, [sds((GROWS, LANE), F32), sds((SMD, LANE), F32), sds((SUB, LANE), F32), sds((SPR, LANE), F32)], [VM] * FOUR)


def finh_kernel(g_ref, sqi_ref, o_ref, sq_ref, sp_ref):
    me = lax.axis_index(AX)
    go = untile(g_ref, o_ref, me, UR // TWO)

    @on(me < ND // TWO)
    def _():
        sq_ref[:] = go(D // LANE, sqi_ref[:])

    @on(me >= ND // TWO)
    def _():
        sq_ref[:] = go(C // LANE, sqi_ref[:])

    sp_ref[:] = o_ref[RSH:RSH + SPR, :]


def finh(g, sqi):
    return run(finh_kernel, (g, sqi), [VM] * TWO, [sds((GROWS, LANE), F32), sds((SUB, LANE), F32), sds((SPR, LANE), F32)], [VM] * THREE)


def tail_kernel(xb, g_ref, sqi_ref, gl_ref, o_ref, sca_ref, rb, sb, sqb, sqa, ss, rs, ss2, rs2, ss5, rs5, ss7, rs7):
    me = entry_barrier()

    def part(q):
        return xb.at[pl.ds(pl.multiple_of(q * TP, SUB), TP)]

    cs = []
    for d in range(ONE, ND):
        peer = lax.rem(me + d, ND)
        c = rcopy(part(peer), rb.at[me], ss.at[d], rs.at[d], peer)
        c.start()
        cs.append(c)
    rb[me] = xb[pl.ds(pl.multiple_of(me * TP, SUB), TP), :]
    go = untile(g_ref, gl_ref, me)

    @on(me < ND // TWO)
    def _():
        sqb[:] = go(D // LANE, sqi_ref[:])

    @on(me >= ND // TWO)
    def _():
        sqb[:] = go(C // LANE, sqi_ref[:])

    wait_all(cs)
    a = rb[ZERO]
    for k in range(ONE, ND):
        a = a + rb[k]
    sb[:] = a
    sqb[:] += sum8(a * a)
    csq = ag_all(me, sqb, sqa, ss7, rs7)
    sqa[me] = sqb[:]

    def to_first():
        return rcopy(sb, o_ref.at[me], ss2, rs2.at[me], ZERO)

    def to_last():
        return rcopy(sb, o_ref.at[me], ss5, rs5.at[me], ND - ONE)

    @on(me != ZERO)
    def _():
        to_first().start()

    @on(me != ND - ONE)
    def _():
        to_last().start()

    o_ref[me] = sb[:]
    wait_all(csq)
    t = sqa[ZERO]
    for k in range(ONE, ND):
        t = t + sqa[k]
    t = jnp.sum(jnp.sum(t, axis=ZERO, keepdims=True), axis=ONE, keepdims=True)
    sca_ref[:] = jnp.broadcast_to(1.0 / jnp.maximum(1.0, jnp.sqrt(t)), (SUB, LANE))

    @on(me != ZERO)
    def _():
        to_first().wait_send()

    @on(me != ND - ONE)
    def _():
        to_last().wait_send()

    @on(me == ZERO)
    def _():
        for d in range(ONE, ND):
            rcopy(sb, o_ref.at[d], ss2, rs2.at[d], ZERO).wait_recv()

    @on(me == ND - ONE)
    def _():
        for d in range(ND - ONE):
            rcopy(sb, o_ref.at[d], ss5, rs5.at[d], ZERO).wait_recv()


def tail(x, g, sqi, cid):
    n = (ND,)
    return run(tail_kernel, (x, g, sqi), [VM] * THREE,
        [sds((GROWS, LANE), F32), sds((ND, TP, LANE), F32), sds((SUB, LANE), F32)], [VM] * THREE,
        scratch=[pltpu.VMEM((ND, TP, LANE), F32), pltpu.VMEM((TP, LANE), F32), pltpu.VMEM((SUB, LANE), F32), pltpu.VMEM((ND, SUB, LANE), F32),
            SEM(n), SEM(n), SEM, SEM(n), SEM, SEM(n), SEM(n), SEM(n)], cid=cid, vlim=VTAIL, flops=40 * TEN**9)


def adam_math(p, m, v, g, decay):
    m2 = BETA_ONE * m + (1.0 - BETA_ONE) * g
    v2 = BETA_TWO * v + (1.0 - BETA_TWO) * g * g
    mh = m2 * (1.0 / (1.0 - BETA_ONE ** ADAM_STEP))
    vh = v2 * (1.0 / (1.0 - BETA_TWO ** ADAM_STEP))
    return p - LEARN_RATE * (mh / (jnp.sqrt(vh) + ADAM_EPS) + decay * p), m2, v2


ABR = 2800
NAB = -(-RSH // ABR)


def head_adam_kernel(sc_ref, dl_ref, pc_ref, p_ref, m_ref, v_ref, po_ref, mo_ref, vo_ref):
    g = dot(dl_ref[:], pc_ref[:]) * sc_ref[ZERO, ZERO]
    po_ref[:], mo_ref[:], vo_ref[:] = adam_math(p_ref[:], m_ref[:], v_ref[:], g, WEIGHT_DECAY)


def head_adam(sc, dl, pc, p, m, v):
    blk = pl.BlockSpec((HAA, LANE), lambda i: (i, ZERO))
    return run(head_adam_kernel, (sc, dl, pc, p, m, v), [SMEM, pl.BlockSpec((HAA, NIMG), lambda i: (i, ZERO)), fixed((NIMG, LANE)), blk, blk, blk],
        [sds(p.shape, F32)] * THREE, [blk] * THREE, grid=-(-NCLS // HAA), flops=30 * TEN**9, nbytes=8 * TEN**7)


def layer_adam_kernel(sc_ref, g0_ref, h0_ref, g1_ref, t0_ref, t1_ref, s0_ref, s1_ref, p_ref, m_ref, v_ref, po_ref, mo_ref, vo_ref, gs):
    k = lax.axis_index(AX)
    i = pl.program_id(ZERO)
    off = TOKR - STEPR * k
    sc = sc_ref[ZERO, ZERO]
    lays = ((g0_ref, t0_ref, s0_ref), (g1_ref, t1_ref, s1_ref))
    ri = i * ABR + lax.broadcasted_iota(jnp.int32, (ABR, LANE), ZERO)
    gs[pl.ds(ZERO, ABR, stride=TWO), :] = jnp.where(ri < off + UR // TWO, g0_ref[:], h0_ref[:]) * sc
    gs[pl.ds(ONE, ABR, stride=TWO), :] = g1_ref[:] * sc
    for b in range(-(-TOKR // ABR)):
        @on(i == b)
        def _():
            n = min(ABR, TOKR - b * ABR)
            r = b * ABR + lax.broadcasted_iota(jnp.int32, (n, LANE), ZERO)
            for l in range(TWO):
                g_ref, t_ref, s_ref = lays[l]
                e = min(n, SPR - b * ABR)
                sp = s_ref[b * ABR:b * ABR + e, :]
                if e < n:
                    sp = jnp.concatenate([sp, jnp.zeros((n - e, LANE), F32)], axis=ZERO)
                alt = jnp.where(k == ZERO, t_ref[b * ABR:b * ABR + n, :], sp)
                gs[pl.ds(l, n, stride=TWO), :] = jnp.where(r < off, alt, g_ref[:n, :]) * sc

    @on(jnp.logical_and(i == NAB - ONE, k == ND - ONE))
    def _():
        r0 = RSH - SMR - (NAB - ONE) * ABR
        for l in range(TWO):
            gs[pl.ds(TWO * r0 + l, SMR, stride=TWO), :] = lays[l][ONE][TOKR:TOKR + SMR, :] * sc

    n2 = TWO * ABR
    r2 = TWO * (RSH * k + i * ABR) + lax.broadcasted_iota(jnp.int32, (n2, LANE), ZERO)
    decay = jnp.where(r2 < TWO * MATR, WEIGHT_DECAY, 0.0)
    a, b, c = adam_math(p_ref.reshape(n2, LANE)[:], m_ref.reshape(n2, LANE)[:], v_ref.reshape(n2, LANE)[:], gs[:], decay)
    po_ref.reshape(n2, LANE)[:] = a
    mo_ref.reshape(n2, LANE)[:] = b
    vo_ref.reshape(n2, LANE)[:] = c


def layer_adam(sc, g0, h0, g1, t0, t1, s0, s1, p, m, v):
    blk = pl.BlockSpec((ABR, TWO, LANE), lambda i: (i, ZERO, ZERO))
    gb = pl.BlockSpec((ABR, LANE), lambda i: (i, ZERO))
    return run(layer_adam_kernel, (sc, g0, h0, g1, t0, t1, s0, s1, p, m, v),
        [SMEM, gb, gb, gb] + [fixed(t.shape) for t in (t0, t1, s0, s1)] + [blk] * THREE, [sds(p.shape, F32)] * THREE, [blk] * THREE,
        scratch=[pltpu.VMEM((TWO * ABR, LANE), F32)], grid=NAB, nbytes=6 * TEN**7)


def solution(mesh):
    row_spec = P(AX)
    layer_spec = P(None, AX)
    in_specs = (row_spec, row_spec, layer_spec, row_spec, row_spec, layer_spec, row_spec, row_spec, layer_spec, row_spec, row_spec)
    out_specs = (P(),) + in_specs[TWO:]
    up = [(i, (i + ONE) % ND) for i in range(ND)]

    def scatter(grad, n):
        return lax.psum_scatter(grad.reshape(ND, n, LANE), AX, scatter_dimension=ZERO, tiled=True).reshape(n // SUB, SUB, LANE)

    def device_step(act_in, labels, layer_p, head_w, small_p, layer_m, head_m, small_m, layer_v, head_v, small_v):
        me = lax.axis_index(AX)
        p3 = rows3(layer_p)
        lab = jnp.pad(labels.astype(F32)[None, :], ((ZERO, SUB - ONE), (ZERO, LANE - B)))
        misc = jnp.concatenate([small_p.reshape(SMD, LANE), lab], axis=ZERO)
        t0, t1, sh0, sh1, toks, tok1, sms, left0, left1 = prep(p3)
        sh1 = lax.ppermute(sh1, AX, [(b, a) for a, b in up])
        t0, tok0, sm_all, misc_all = start(sh0, toks, sms, misc, left0, t0, ONE)
        t1 = fix(sh1, left1, t1)
        wg = []
        for t in (t0, t1):
            wg.append(lax.all_gather(t, AX, tiled=True))
        tok1 = lax.psum(tok1, AX)
        wp = [wprep(ZERO, tok0, sm_all, misc_all)]
        hidden = act_in
        saved = []
        for l in range(TWO):
            x1, n2, ta, tg = tok_fwd(hidden, wp[l])
            if l == ZERO:
                hw, x1 = lax.optimization_barrier((head_w, x1))
                wall = lax.all_gather(hconv(hw.T), AX)
                wp.append(wprep(ONE, tok1, sm_all, misc_all))
            x1 = x1.reshape(T, C)
            n2 = n2.reshape(T, C)
            x2, act, gp, *pooled = ch_fwd(n2, x1, wg[l], wp[l], l)
            saved.append((hidden, ta, tg, x1, n2, act, gp))
            hidden = x2.reshape(B, SP, C)
        dl, gb, loss, dpool, pall, sqh = head(wall, pooled[ZERO], wp[ZERO], TWO)
        dl_all = lax.all_gather(dl, AX, tiled=True)
        pc = lax.dynamic_slice_in_dim(pall.reshape(NIMG, C), LANE * me, LANE, axis=ONE)
        for l in (ONE, ZERO):
            hid_in, ta, tg, x1, n2, act, gp = saved[l]
            if l:
                dh, dbc1, dbc2, d_out, dgf, dsf = ch_bwd_top(x2, dpool, gp, wg[l], wp[l])
                dh, dl_all = lax.optimization_barrier((dh, dl_all))
                grad = dw1_call(n2, dh, dw2_call(act, d_out))
                dh, grad = lax.optimization_barrier((dh, grad))
                shard1 = scatter(grad, UR)
            else:
                g2 = dw2_call(act, d_out, ONE)
                g2, d_out = lax.optimization_barrier((g2, d_out))
                dh, dbc1, dbc2 = ch_bwd_a(d_out, gp, wg[l])
                dh, tot = lax.optimization_barrier((dh, tot))
                grad = dw1_call(n2, dh, g2, ONE)
                dh, grad, tot, act = lax.optimization_barrier((dh, grad, tot, act))
                shard_b = scatter(grad, UR // TWO)
                gl1, small_g, sq, sp1 = fin(shard1, tot, sqh)
                sp1 = lax.ppermute(sp1, AX, up)
                dh, sq, act = lax.optimization_barrier((dh, sq, act))
                grad = dw1_call(n2, dh, dw2_call(act, d_out, ZERO), ZERO)
                dh, grad = lax.optimization_barrier((dh, grad))
                shard_a = scatter(grad, UR // TWO)
            da, dg2, ds2 = ch_bwd_b(dh, wg[l], x1, d_out, wp[l])
            if l == ZERO:
                h0, sq, sp0 = finh(shard_b, sq)
                sp0 = lax.ppermute(sp0, AX, up)
                da, sq = lax.optimization_barrier((da, sq))
            o = tok_bwd(hid_in, da.reshape(B, SP, C), ta, tg, wp[l], l)
            if l:
                d_out = o[ZERO].reshape(T, C)
                o = o[ONE:]
            parts = tuple(o) + (dg2, ds2, dbc1, dbc2)
            if l:
                sv, d_out = lax.optimization_barrier((pack(parts, (gb, dgf, dsf)), d_out))
                tot = lax.psum(sv, AX)
        px, sp0 = lax.optimization_barrier((pack(parts), sp0))
        gl0, tsm, sca = tail(px, shard_a, sq, FOUR)
        np3, nm3, nv3 = layer_adam(sca, gl0, h0, gl1, tsm.reshape(ND * TP, LANE), tot, sp0, sp1, p3, rows3(layer_m), rows3(layer_v))
        nh, nhm, nhv = head_adam(sca, dl_all, pc, head_w.T, head_m.T, head_v.T)
        nsp, nsm, nsv = adam_math(small_p, small_m, small_v, small_g.reshape(SMD * LANE) * sca[ZERO, ZERO], 0.0)
        return (loss[ZERO, ZERO], unrows3(np3), nh.T, nsp, unrows3(nm3), nhm.T, nsm, unrows3(nv3), nhv.T, nsv)

    return jax.shard_map(device_step, mesh=mesh, in_specs=in_specs, out_specs=out_specs, check_vma=False)
```

```python
import functools
import math
import jax
import jax.numpy as jnp
from jax import lax
from jax.experimental import pallas as pl
from jax.experimental.pallas import tpu as pltpu
from jax.experimental.layout import with_layout_constraint, Layout
from jax.sharding import PartitionSpec as P


F32 = jnp.float32
BF = jnp.bfloat16
LN_EPS = 1e-6
LEARN_RATE = 0.003
BETA_ONE = 0.9
BETA_TWO = 0.999
ADAM_EPS = 1e-8
WEIGHT_DECAY = 0.03
ADAM_STEP = 10
GC0 = math.sqrt(2 / math.pi)
GC1 = GC0 * 0.044715

LANE = 128
SUB = 8
ND = 8
AX = 'fsdp'
B = 32
S = 196
SP = 200
C = 1024
J = 512
D = 4096
NCLS = 21843
NIMG = 256
T = B * SP
KC = 2816
KR = KC // LANE
RSH = 8398
TOKR = 1568
HTOK = TOKR // 2
UNIT = 512
NU = 16
UR = UNIT * NU
STEPR = RSH - UR
SPILL = TOKR - STEPR
SPR = SPILL + 6
MATR = TOKR + ND * UR
SMR = 80
GROWS = RSH + SPILL + SUB
TP = 208
SMF = 192
SMD = SMF // ND
VROW = 16
VLIM = 64 * 1024 * 1024 - 65536
VTAIL = 16 * 1024 * 1024
NT = (((1,), (1,)), ((), ()))
TN = (((0,), (0,)), ((), ()))
VM = pl.BlockSpec(memory_space=pltpu.VMEM)
HBM = pl.BlockSpec(memory_space=pl.ANY)
SMEM = pl.BlockSpec(memory_space=pltpu.SMEM)
SEM = pltpu.SemaphoreType.DMA
VG1, VS1, VG2, VS2, VB2, VB1, VLG, VLS = 0, 1, 2, 3, 4, 5, 9, 10


ZERO, ONE, TWO, THREE, FOUR, TEN = 0, 1, 2, 3, 4, 10


def sds(shape, dt):
    return jax.ShapeDtypeStruct(shape, dt)


def fixed(shape, idx=None, once=False):
    ix = tuple(idx) if idx else (0,) * len(shape)
    return pl.BlockSpec(shape, lambda i: ix, pipeline_mode=pl.Buffered(1) if once else None)


def run(body, ins, in_specs, outs, out_specs, scratch=(), grid=None, flops=10**9, nbytes=10**6, alias={}, cid=None, vlim=VLIM):
    kw = dict(vmem_limit_bytes=vlim)
    if cid is not None:
        kw.update(collective_id=cid, has_side_effects=True)
    if grid:
        kw.update(dimension_semantics=("arbitrary",))
    extra = dict(grid=(grid,)) if grid else {}
    return pl.pallas_call(body, in_specs=in_specs, out_specs=out_specs, out_shape=outs, scratch_shapes=list(scratch),
        input_output_aliases=alias, cost_estimate=pl.CostEstimate(flops=flops, bytes_accessed=nbytes, transcendentals=0),
        compiler_params=pltpu.CompilerParams(**kw), **extra)(*ins)


def on(cond):
    return pl.when(cond)


def unit_stats(xf):
    mean = jnp.sum(xf, axis=-ONE, keepdims=True) * (1.0 / C)
    xc = xf - mean
    rstd = lax.rsqrt(jnp.sum(xc * xc, axis=-ONE, keepdims=True) * (1.0 / C) + LN_EPS)
    return xc * rstd, rstd


def sum8(v):
    return jnp.sum(v.reshape(v.shape[ZERO] // SUB, SUB, v.shape[ONE]), axis=ZERO)


def ln_bwd(nh, rstd, dy, g):
    dxh = dy * g
    m1 = jnp.sum(dxh, axis=-ONE, keepdims=True) * (1.0 / C)
    m2 = jnp.sum(dxh * nh, axis=-ONE, keepdims=True) * (1.0 / C)
    return rstd * (dxh - m1 - nh * m2)


def gelu_both(h):
    u = h * h
    t = jnp.tanh(h * (GC0 + GC1 * u))
    cdf = 0.5 + 0.5 * t
    a = h * cdf
    return a.astype(BF), cdf + (a * (1.0 - t)) * (GC0 + (THREE * GC1) * u)


def wcols(w_ref, c0, n):
    r = w_ref.shape[ZERO] * 16
    return jnp.concatenate([w_ref[:, j].reshape(r, LANE) for j in range(c0 // LANE, (c0 + n) // LANE)], axis=ONE)


def wrows(w_ref, r0, n):
    return jnp.concatenate([w_ref[r0 // 16:(r0 + n) // 16, j].reshape(n, LANE) for j in range(w_ref.shape[ONE])], axis=ONE)


def dot(a, b):
    return jnp.dot(a, b, preferred_element_type=F32)


def dotg(a, b, dn):
    return lax.dot_general(a, b, dn, preferred_element_type=F32)


def entry_barrier():
    me = lax.axis_index(AX)
    b = pltpu.get_barrier_semaphore()
    for d in range(ONE, ND):
        pl.semaphore_signal(b, inc=ONE, device_id=(lax.rem(me + d, ND),), device_id_type=pl.DeviceIdType.MESH)
    pl.semaphore_wait(b, ND - ONE)
    return me


def rcopy(src, dst, ss, rs, dev):
    return pltpu.make_async_remote_copy(src_ref=src, dst_ref=dst, send_sem=ss, recv_sem=rs, device_id=(dev,), device_id_type=pl.DeviceIdType.MESH)


def ag_all(me, src, dst, ss, rs):
    cs = []
    for d in range(ONE, ND):
        c = rcopy(src, dst.at[me], ss.at[d], rs.at[d], lax.rem(me + d, ND))
        c.start()
        cs.append(c)
    return cs


def wait_all(cs):
    for c in cs:
        c.wait()


def rows3(a):
    b = with_layout_constraint(a.reshape(TWO, RSH, LANE), Layout(major_to_minor=(ONE, ZERO, TWO)))
    return b.transpose(ONE, ZERO, TWO)


def unrows3(a):
    b = with_layout_constraint(a.transpose(ONE, ZERO, TWO), Layout(major_to_minor=(ONE, ZERO, TWO)))
    return b.reshape(TWO, RSH * LANE)


OWN = NU - THREE
LEFT = RSH - (TOKR - STEPR * (ND - ONE)) - UNIT * OWN
NTILE = UNIT // 16


def tiles(o_ref, src, r0, step_rows, nj, n, t0):
    def step(i, _):
        for j in range(nj):
            o_ref[t0 + i * nj + j] = src[pl.ds(r0 + (i * 16 * nj + j) * step_rows, 16, stride=nj * step_rows), :].astype(BF)
        return ZERO

    lax.fori_loop(ZERO, n * NTILE // nj, step, ZERO)


def by_half(me, f):
    @on(me < ND // TWO)
    def _():
        f(D // LANE)

    @on(me >= ND // TWO)
    def _():
        f(C // LANE)


TQ = TOKR // ND
HCH = FOUR
HAB = ND * KC // HCH


def prep_kernel(p_ref, o0_ref, o1_ref, shs0_ref, shs1_ref, toks_ref, tok1_ref, sms_ref, left0_ref, left1_ref):
    me = lax.axis_index(AX)
    src = p_ref.reshape(TWO * RSH, LANE)
    for l in range(TWO):
        (shs0_ref, shs1_ref)[l][:] = src[pl.ds(l, SPR, stride=TWO), :].astype(BF)
        (left0_ref, left1_ref)[l][:] = src[pl.ds(TWO * (RSH - LEFT) + l, LEFT, stride=TWO), :]
        sms_ref[l] = src[pl.ds(TWO * (RSH - SMR) + l, SMR, stride=TWO), :].astype(BF)
    off = TOKR - STEPR * me

    def go(nj):
        for l in range(TWO):
            tiles((o0_ref, o1_ref)[l], src, TWO * off + l, TWO, nj, OWN, ZERO)

    by_half(me, go)

    @on(me == ZERO)
    def _():
        for q in range(ND):
            toks_ref[q] = src[pl.ds(TWO * TQ * q, TQ, stride=TWO), :].astype(BF)
        tok1_ref[:] = src[pl.ds(ONE, TOKR, stride=TWO), :].astype(BF).astype(F32)

    @on(me != ZERO)
    def _():
        toks_ref[:] = jnp.zeros(toks_ref.shape, BF)
        tok1_ref[:] = jnp.zeros(tok1_ref.shape, F32)


def prep(p3):
    tile = sds((NU * NTILE, 16, LANE), BF)
    sh = sds((SPR, LANE), BF)
    left = sds((LEFT, LANE), F32)
    return run(prep_kernel, (p3,), [VM], [tile, tile, sh, sh, sds((ND, TQ, LANE), BF), sds((TOKR, LANE), F32), sds((TWO, SMR, LANE), BF), left, left], [VM] * 9)


def last_units(me, left_ref, shr_ref, z, w):
    z[:LEFT, :] = left_ref[:]
    z[LEFT:, :] = shr_ref[:].astype(F32)
    r0 = LEFT - (RSH - (TOKR - STEPR * me) - UNIT * OWN)
    by_half(me, lambda nj: tiles(w, z, r0, ONE, nj, NU - OWN, ZERO))


def put_last(w, o_ref, sem):
    c = pltpu.make_async_copy(w, o_ref.at[pl.ds(OWN * NTILE, (NU - OWN) * NTILE)], sem)
    c.start()
    return c


LAST_SCR = [pltpu.VMEM((LEFT + SPR, LANE), F32), pltpu.VMEM(((NU - OWN) * NTILE, 16, LANE), BF)]


def fix_kernel(shr_ref, left_ref, u_ref, o_ref, z, w, sem):
    last_units(lax.axis_index(AX), left_ref, shr_ref, z, w)
    put_last(w, o_ref, sem).wait()


def fix(shr, left, t):
    return run(fix_kernel, (shr, left, t), [VM, VM, HBM], sds(t.shape, BF), HBM, scratch=LAST_SCR + [SEM], alias={TWO: ZERO})


def start_kernel(shs, toks, sms, misc_ref, left_ref, u_ref, hw_ref, o_ref, tok_o, sm_o, misc_o, hb_ref, hin, hout, hsem, z, w, shr, ss_m, rs_m, ss_s, rs_s, ss_t, rs_t, ss_u, ss_h, rs_h, ss_w):
    rows = [min(HAB, NCLS - k * HAB) for k in range(HCH)]
    cin = [pltpu.make_async_copy(hw_ref.at[pl.ds(k * HAB, n)], hin.at[k, pl.ds(ZERO, n)], hsem.at[ZERO, k]) for k, n in enumerate(rows)]
    cout = [pltpu.make_async_copy(hout.at[k], hb_ref.at[pl.ds(k * HAB, HAB)], hsem.at[ONE, k]) for k in range(HCH)]
    for c in cin:
        c.start()
    me = entry_barrier()
    sh = rcopy(shs, shr, ss_h, rs_h, lax.rem(me + ND - ONE, ND))
    sh.start()

    def first_send(d):
        return rcopy(toks.at[d], tok_o.at[d], ss_t.at[d], rs_t.at[d], d)

    def zero_send(d):
        return rcopy(toks.at[ZERO], tok_o.at[ZERO], ss_u.at[d], rs_t.at[ZERO], d)

    def piece(q, d):
        return rcopy(tok_o.at[q], tok_o.at[q], ss_t.at[d], rs_t.at[q], lax.rem(me - ONE + d, ND - ONE) + ONE)

    def small(d):
        return rcopy(sms, sm_o, ss_s.at[d], rs_s, d)

    @on(me == ZERO)
    def _():
        for d in range(ONE, ND):
            first_send(d).start()
        for d in range(ONE, ND):
            zero_send(d).start()
        tok_o[:] = toks[:]

    @on(me == ND - ONE)
    def _():
        for d in range(ND - ONE):
            small(d).start()
        sm_o[:] = sms[:]

    csm = ag_all(me, misc_ref, misc_o, ss_m, rs_m)
    misc_o[me] = misc_ref[:]

    @on(me > ZERO)
    def _():
        piece(me, ZERO).wait_recv()
        for d in range(ONE, ND - ONE):
            piece(me, d).start()

    for k in range(HCH):
        cin[k].wait()
        v = hin[k]
        if rows[k] < HAB:
            v = jnp.where(lax.broadcasted_iota(jnp.int32, (HAB, LANE), ZERO) < rows[k], v, 0.0)
        hout[k] = v.astype(BF)
        cout[k].start()
    sh.wait()
    last_units(me, left_ref, shr, z, w)
    cw = put_last(w, o_ref, ss_w)
    wait_all(csm)

    @on(me < ND - ONE)
    def _():
        small(ZERO).wait_recv()

    @on(me > ZERO)
    def _():
        for d in range(ND - ONE):
            piece(lax.rem(me + ONE + d, ND), ZERO).wait_recv()
        for d in range(ONE, ND - ONE):
            piece(me, d).wait_send()

    @on(me == ZERO)
    def _():
        for d in range(ONE, ND):
            first_send(d).wait_send()
            zero_send(d).wait_send()

    @on(me == ND - ONE)
    def _():
        for d in range(ND - ONE):
            small(d).wait_send()

    cw.wait()
    wait_all(cout)


def start(shs, toks, sms, misc, left, t, hw, cid):
    n = (ND,)
    return run(start_kernel, (shs, toks, sms, misc, left, t, hw), [VM] * 5 + [HBM] * TWO,
        [sds(t.shape, BF), sds(toks.shape, BF), sds(sms.shape, BF), sds(n + misc.shape, F32), sds((ND * KC, LANE), BF)], [HBM] + [VM] * THREE + [HBM],
        scratch=[pltpu.VMEM((HCH, HAB, LANE), F32), pltpu.VMEM((HCH, HAB, LANE), BF), SEM((TWO, HCH))] + LAST_SCR + [pltpu.VMEM((SPR, LANE), BF), SEM(n), SEM(n), SEM(n), SEM, SEM(n), SEM(n), SEM(n), SEM, SEM, SEM],
        alias={5: ZERO}, flops=TEN**TEN, cid=cid)


def shift_pick(a, b, lane, r):
    return jnp.where(lane < LANE - r, pltpu.roll(a, (LANE - r) % LANE, ONE), pltpu.roll(b, (LANE - r) % LANE, ONE))


def wprep_kernel(l, tok_ref, sm_ref, misc_ref, w1a_ref, w1t_ref, w2p_ref, w2t_ref, b2c_ref, vec_ref, *rest):
    tf, w1s, w2l, w2h, sf, sg = rest[-6:]
    me = lax.axis_index(AX)
    for k in range(ND):
        sf[k * SMD:(k + ONE) * SMD, :] = misc_ref[k, :SMD, :].astype(BF).astype(F32)
    if l == ZERO:
        lab_ref, bias_ref = rest[:TWO]
        for k in range(ND):
            lab_ref[:, k * B:(k + ONE) * B] = jnp.broadcast_to(misc_ref[k, SMD:SMD + ONE, :B], (SUB, B))
            tf[k * TQ:(k + ONE) * TQ, :] = tok_ref[k].astype(F32)
        bias_ref[:] = jnp.zeros(bias_ref.shape, F32)
        bias_ref[:KR, :] = sf[pl.ds(16 + KR * me, KR), :]
    else:
        tf[:TOKR, :] = tok_ref[:]
    vec_ref[:] = jnp.zeros(vec_ref.shape, F32)
    w1s[:] = jnp.zeros(w1s.shape, F32)
    lane = lax.broadcasted_iota(jnp.int32, (16, LANE), ONE)

    def put(row, src, r0, n):
        for i in range(n):
            vec_ref[ZERO, row + i // SUB:row + i // SUB + ONE, (i % SUB) * LANE:(i % SUB + ONE) * LANE] = src[r0 + i:r0 + i + ONE, :]

    smf = sm_ref[l].astype(F32)
    sg[:SMR, :] = smf
    for j in range(FOUR):
        w1s[:S, j * LANE:(j + ONE) * LANE] = tf[pl.ds(j, S, stride=FOUR), :]
        w1s[S:S + ONE, j * LANE:(j + ONE) * LANE] = sg[16 + j:17 + j, :]
    for b in range(32):
        p = S * b
        r0 = HTOK + p // LANE
        o = p % LANE
        x = [tf[pl.ds(r0 + q, 16, stride=49), :] for q in range(THREE if o + S > TWO * LANE else TWO)]
        w2l[pl.ds(b, 16, stride=32), :] = shift_pick(x[ZERO], x[ONE], lane, o)
        hi = shift_pick(x[ONE], x[-ONE], lane, o)
        w2h[pl.ds(b, 16, stride=32), :] = jnp.where(lane < S - LANE, hi, 0.0)
    w1 = w1s[:]
    w2 = jnp.concatenate([w2l[:], w2h[:]], axis=ONE)
    w1a_ref[ZERO] = w1[:SP].astype(BF)
    w1t_ref[ZERO] = w1.T[:, :SP].astype(BF)
    w2p_ref[ZERO] = w2[:, :SP].astype(BF)
    w2t_ref[ZERO] = w2.T[:SP].astype(BF)
    put(VG1, sg, ZERO, SUB)
    put(VS1, sg, SUB, SUB)
    b2 = jnp.concatenate([sg[20:21, :], sg[21:22, :]], axis=ONE)
    b2 = jnp.broadcast_to(b2, (SUB, TWO * LANE)).T[:SP, :ONE]
    rowi = lax.broadcasted_iota(jnp.int32, (SP, LANE), ZERO)
    b2c_ref[ZERO] = jnp.where(rowi < S, jnp.broadcast_to(b2, (SP, LANE)), 0.0)
    lane7 = lax.broadcasted_iota(jnp.int32, (56, LANE), ONE)
    sg[:56, :] = shift_pick(smf[21:77], smf[22:78], lane7, S - LANE)
    put(VG2, sg, ZERO, SUB)
    put(VS2, sg, SUB, SUB)
    put(VB1, sg, 16, 32)
    put(VB2, sg, 48, SUB)
    put(VLG, sf, ZERO, SUB)
    put(VLS, sf, SUB, SUB)


def wprep(l, tok, sm, misc):
    extra = [] if l else [sds((SUB, NIMG), F32), sds((24, LANE), F32)]
    outs = [sds((ONE, SP, J), BF), sds((ONE, J, SP), BF), sds((ONE, J, SP), BF), sds((ONE, SP, J), BF), sds((ONE, SP, LANE), F32), sds((ONE, VROW, C), F32)] + extra
    return run(functools.partial(wprep_kernel, l), (tok, sm, misc), [VM] * THREE, outs, [VM] * len(outs),
        scratch=[pltpu.VMEM((TOKR + SUB, LANE), F32), pltpu.VMEM((256, J), F32), pltpu.VMEM((J, LANE), F32), pltpu.VMEM((J, LANE), F32), pltpu.VMEM((SMF, LANE), F32), pltpu.VMEM((SMR, LANE), F32)],
        flops=5 * TEN**9)


def vec_spec():
    return fixed((ONE, VROW, C))


def lay(shape):
    return fixed((ONE,) + shape)


CW = 256


def tok_fwd_kernel(x_ref, w1t_ref, w2t_ref, b2_ref, v_ref, out_ref, n2_ref, act_ref, gp_ref, n_s):
    @on(pl.program_id(ZERO) == ZERO)
    def _():
        r = lax.broadcasted_iota(jnp.int32, (SP, C), ZERO)
        for im in range(TWO):
            n_s[im] = jnp.where(r == S, 1.0, 0.0).astype(BF)

    for im in range(TWO):
        xf = x_ref[im, :S, :].astype(F32)
        nh, _ = unit_stats(xf)
        n_s[im, :S, :] = (nh * v_ref[ZERO, VG1:VG1 + ONE, :] + v_ref[ZERO, VS1:VS1 + ONE, :]).astype(BF)
    for im in range(TWO):
        cols = []
        for c in range(ZERO, C, CW):
            cs = slice(c, c + CW)
            a, gp = gelu_both(dot(w1t_ref[ZERO], n_s[im, :, cs]))
            act_ref[im, :, cs] = a
            gp_ref[im, :, cs] = gp
            o = dot(w2t_ref[ZERO], a) + b2_ref[ZERO, :, :ONE]
            cols.append((x_ref[im, :S, cs].astype(F32) + o[:S]).astype(BF))
        x1 = jnp.concatenate(cols, axis=ONE)
        out_ref[im, :S, :] = x1
        nh2, _ = unit_stats(x1.astype(F32))
        n2_ref[im, :S, :] = (nh2 * v_ref[ZERO, VG2:VG2 + ONE, :] + v_ref[ZERO, VS2:VS2 + ONE, :]).astype(BF)
        out_ref[im, S:, :] = jnp.zeros((SP - S, C), BF)
        n2_ref[im, S:, :] = jnp.zeros((SP - S, C), BF)


def img(r, n=C):
    return pl.BlockSpec((TWO, r, n), lambda i: (i, ZERO, ZERO))


def tok_fwd(x, wp):
    return run(tok_fwd_kernel, (x, wp[ONE], wp[THREE], wp[FOUR], wp[5]),
        [img(x.shape[ONE]), lay((J, SP)), lay((SP, J)), lay((SP, LANE)), vec_spec()],
        [sds((B, SP, C), BF)] * TWO + [sds((B, J, C), BF), sds((B, J, C), F32)], [img(SP)] * TWO + [img(J)] * TWO,
        scratch=[pltpu.VMEM((TWO, SP, C), BF)], grid=B // TWO, flops=60 * TEN**9, nbytes=14 * TEN**7)


def tok_bwd_kernel(need_dx, x_ref, da_ref, act_ref, gp_ref, w1a_ref, w2p_ref, v_ref, *rest):
    if need_dx:
        dx_ref = rest[ZERO]
        rest = rest[ONE:]
    dw1_ref, dw2_ref, db1_ref, db2_ref, dg_ref, ds_ref, n_s, nh_s, dh_s, dn_s = rest

    @on(pl.program_id(ZERO) == ZERO)
    def _():
        for r in (dw1_ref, dw2_ref, db1_ref, db2_ref, dg_ref, ds_ref, n_s):
            r[:] = jnp.zeros(r.shape, r.dtype)

    rs = []
    for im in range(TWO):
        nh, rstd = unit_stats(x_ref[im, :S, :].astype(F32))
        nh_s[im, :S, :] = nh
        rs.append(rstd)
        n_s[:S, im * C:(im + ONE) * C] = (nh * v_ref[ZERO, VG1:VG1 + ONE, :] + v_ref[ZERO, VS1:VS1 + ONE, :]).astype(BF)
    db1 = db1_ref[:]
    for im in range(TWO):
        for c in range(ZERO, C, CW):
            cs = slice(c, c + CW)
            dact = dot(w2p_ref[ZERO], da_ref[im, :, cs]).astype(BF).astype(F32)
            dh = dact * gp_ref[im, :, cs]
            for k in range(ZERO, CW, LANE):
                db1 = db1 + dh[:, k:k + LANE]
            dhb = dh.astype(BF)
            dh_s[:, im * C + c:im * C + c + CW] = dhb
            dn_s[im, :, cs] = dot(w1a_ref[ZERO], dhb)
    db1_ref[:] = db1
    act2 = jnp.concatenate([act_ref[ZERO], act_ref[ONE]], axis=ONE)
    da2 = jnp.concatenate([da_ref[ZERO], da_ref[ONE]], axis=ONE)
    dw2_ref[:] += dotg(act2, da2, NT)
    dw1_ref[:] += dotg(dh_s[:], n_s[:], NT)
    db2 = db2_ref[:]
    s8 = S // SUB * SUB
    for im in range(TWO):
        for k in range(ZERO, C, LANE):
            db2 = db2 + da_ref[im, :, k:k + LANE].astype(F32)
        dn = dn_s[im, :S, :].astype(BF).astype(F32)
        nh = nh_s[im, :S, :]
        pr = dn * nh
        dg_ref[:] += sum8(pr[:s8])
        ds_ref[:] += sum8(dn[:s8])
        dg_ref[:S - s8] += pr[s8:]
        ds_ref[:S - s8] += dn[s8:]
        if need_dx:
            dx = ln_bwd(nh, rs[im], dn, v_ref[ZERO, VG1:VG1 + ONE, :])
            dx_ref[im, :S, :] = (da_ref[im, :S, :].astype(F32) + dx).astype(BF)
            dx_ref[im, S:, :] = jnp.zeros((SP - S, C), BF)
    db2_ref[:] = db2


def tok_bwd(x, da, act, gp, wp, l):
    acc = [(J, SP), (J, SP), (J, LANE), (SP, LANE), (SUB, C), (SUB, C)]
    dx = [sds((B, SP, C), BF)] if l else []
    return run(functools.partial(tok_bwd_kernel, bool(l)), (x, da, act, gp, wp[ZERO], wp[TWO], wp[5]),
        [img(x.shape[ONE]), img(SP), img(J), img(J), lay((SP, J)), lay((J, SP)), vec_spec()],
        dx + [sds(s, F32) for s in acc], [img(SP)] * len(dx) + [fixed(s) for s in acc],
        scratch=[pltpu.VMEM((SP, TWO * C), BF), pltpu.VMEM((TWO, SP, C), F32), pltpu.VMEM((J, TWO * C), BF), pltpu.VMEM((TWO, SP, C), F32)],
        grid=B // TWO, flops=60 * TEN**9, nbytes=14 * TEN**7)


M = 400
DC = 512


def row(n):
    return pl.BlockSpec((M, n), lambda i: (i, ZERO))


def wspec(h):
    return fixed((64, 32, 16, LANE) if h == ZERO else (256, SUB, 16, LANE), (h, ZERO, ZERO, ZERO), True)


def pair(n):
    return pl.BlockSpec((ONE, TWO, n), lambda i: (i, ZERO, ZERO))


def ch_fwd_kernel(n2_ref, x1_ref, w1_ref, w2_ref, v_ref, x2_ref, act_ref, gp_ref, *pool_ref):
    n2 = n2_ref[:]
    for k in range(D // DC):
        ks = slice(k * DC, (k + ONE) * DC)
        r = VB1 + k // TWO
        b = v_ref[ZERO, r:r + ONE, (k % TWO) * DC:(k % TWO + ONE) * DC]
        act_ref[:, ks], gp_ref[:, ks] = gelu_both(dot(n2, wcols(w1_ref, k * DC, DC)) + b)
    for c in range(ZERO, C, CW):
        cs = slice(c, c + CW)
        o = dot(act_ref[:], wcols(w2_ref, c, CW)) + v_ref[ZERO, VB2:VB2 + ONE, cs]
        x2_ref[:, cs] = (x1_ref[:, cs].astype(F32) + o).astype(BF)
    if pool_ref:
        nh, _ = unit_stats(x2_ref[:].astype(F32))
        n = (nh * v_ref[ZERO, VLG:VLG + ONE, :] + v_ref[ZERO, VLS:VLS + ONE, :]).astype(BF).astype(F32)
        for im in range(TWO):
            pool_ref[ZERO][ZERO, im:im + ONE, :] = jnp.sum(n[im * SP:im * SP + S], axis=ZERO, keepdims=True) * (1.0 / S)


def w_views(wg):
    return wg.reshape(128, 32, 16, LANE), wg.reshape(512, SUB, 16, LANE)


def ch_fwd(n2, x1, wg, wp, l):
    return run(ch_fwd_kernel, (n2, x1) + w_views(wg) + (wp[5],), [row(C), row(C), wspec(ZERO), wspec(ONE), vec_spec()],
        [sds((T, C), BF), sds((T, D), BF), sds((T, D), F32)] + [sds((B // TWO, TWO, C), F32)] * l, [row(C), row(D), row(D)] + [pair(C)] * l,
        grid=T // M, flops=FOUR * T * C * D, nbytes=T * D * 6)


def ch_bwd_a_kernel(do_ref, gp_ref, w2_ref, dh_ref, db1_ref, db2_ref):
    @on(pl.program_id(ZERO) == ZERO)
    def _():
        db1_ref[:] = jnp.zeros(db1_ref.shape, F32)
        db2_ref[:] = jnp.zeros(db2_ref.shape, F32)

    do = do_ref[:]
    db2_ref[:] += sum8(do.astype(F32))
    for k in range(D // DC):
        ks = slice(k * DC, (k + ONE) * DC)
        da = dotg(do, wrows(w2_ref, k * DC, DC), NT).astype(BF).astype(F32)
        dh = da * gp_ref[:, ks]
        db1_ref[:, ks] += sum8(dh)
        dh_ref[:, ks] = dh.astype(BF)


def ch_bwd_top_kernel(x2_ref, dp_ref, v_ref, gp_ref, w2_ref, dh_ref, db1_ref, db2_ref, do_ref, dg_ref, ds_ref):
    @on(pl.program_id(ZERO) == ZERO)
    def _():
        dg_ref[:] = jnp.zeros(dg_ref.shape, F32)
        ds_ref[:] = jnp.zeros(ds_ref.shape, F32)

    g = v_ref[ZERO, VLG:VLG + ONE, :]
    r = lax.broadcasted_iota(jnp.int32, (SP, ONE), ZERO)
    xf = x2_ref[:].astype(F32)
    out = []
    for im in range(TWO):
        dn = (dp_ref[ZERO, im:im + ONE, :] * (1.0 / S)).astype(BF).astype(F32)
        nh, rstd = unit_stats(xf[im * SP:(im + ONE) * SP])
        dxh = dn * g
        m1 = jnp.sum(dxh, axis=-ONE, keepdims=True) * (1.0 / C)
        m2 = jnp.sum(dxh * nh, axis=-ONE, keepdims=True) * (1.0 / C)
        out.append(jnp.where(r < S, rstd * ((dxh - m1) - nh * m2), 0.0))
        dg_ref[ZERO:ONE, :] += dn * jnp.sum(nh[:S], axis=ZERO, keepdims=True)
        ds_ref[ZERO:ONE, :] += dn * float(S)
    do_ref[:] = jnp.concatenate(out, axis=ZERO).astype(BF)
    ch_bwd_a_kernel(do_ref, gp_ref, w2_ref, dh_ref, db1_ref, db2_ref)


def ch_bwd_a(do, gp, wg):
    return run(ch_bwd_a_kernel, (do, gp, w_views(wg)[ONE]), [row(C), row(D), wspec(ONE)],
        [sds((T, D), BF), sds((SUB, D), F32), sds((SUB, C), F32)], [row(D), fixed((SUB, D)), fixed((SUB, C))],
        grid=T // M, flops=TWO * T * C * D, nbytes=T * D * 6)


def ch_bwd_top(x2, dp, gp, wg, wp):
    return run(ch_bwd_top_kernel, (x2, dp, wp[5], gp, w_views(wg)[ONE]), [row(C), pair(C), vec_spec(), row(D), wspec(ONE)],
        [sds((T, D), BF), sds((SUB, D), F32), sds((SUB, C), F32), sds((T, C), BF), sds((SUB, C), F32), sds((SUB, C), F32)],
        [row(D), fixed((SUB, D)), fixed((SUB, C)), row(C), fixed((SUB, C)), fixed((SUB, C))],
        grid=T // M, flops=TWO * T * C * D, nbytes=T * D * 6)


def ch_bwd_b_kernel(dh_ref, w1_ref, x1_ref, do_ref, v_ref, da_ref, dg_ref, ds_ref, dn_s):
    @on(pl.program_id(ZERO) == ZERO)
    def _():
        dg_ref[:] = jnp.zeros(dg_ref.shape, F32)
        ds_ref[:] = jnp.zeros(ds_ref.shape, F32)

    for c in range(ZERO, C, CW):
        dn_s[:, c:c + CW] = dotg(dh_ref[:], wrows(w1_ref, c, CW), NT)
    dy = dn_s[:].astype(BF).astype(F32)
    nh, rstd = unit_stats(x1_ref[:].astype(F32))
    dx = ln_bwd(nh, rstd, dy, v_ref[ZERO, VG2:VG2 + ONE, :])
    dg_ref[:] += sum8(dy * nh)
    ds_ref[:] += sum8(dy)
    r = lax.rem(lax.broadcasted_iota(jnp.int32, (M, ONE), ZERO), SP)
    da_ref[:] = jnp.where(r < S, do_ref[:].astype(F32) + dx, 0.0).astype(BF)


def ch_bwd_b(dh, wg, x1, do, wp):
    return run(ch_bwd_b_kernel, (dh, w_views(wg)[ZERO], x1, do, wp[5]), [row(D), wspec(ZERO), row(C), row(C), vec_spec()],
        [sds((T, C), BF)] + [sds((SUB, C), F32)] * TWO, [row(C)] + [fixed((SUB, C))] * TWO,
        scratch=[pltpu.VMEM((M, C), F32)], grid=T // M, flops=TWO * T * C * D, nbytes=T * D * THREE)


def dw2_kernel(a_ref, b_ref, o_ref):
    r = dotg(a_ref[:], b_ref[:], TN)
    for j in range(C // LANE):
        o_ref[ZERO, :, j] = r[:, LANE * j:LANE * (j + ONE)].reshape(DC // SUB, SUB, LANE)


def dw2_call(act, do, h=None):
    q = C // DC
    own = ND // TWO
    full = h is None
    a_spec = pl.BlockSpec((T, DC), (lambda i: (ZERO, i)) if full else (lambda i: (ZERO, q * i + h)))
    o_map = (lambda i: (own + i // q, lax.rem(i, q), ZERO, ZERO, ZERO)) if full else (lambda i: (own + i, ZERO, ZERO, ZERO, ZERO))
    n = C if full else DC
    return run(dw2_kernel, (act, do), [a_spec, fixed((T, C), once=True)],
        sds((ND, n // SUB, SUB, SUB, LANE), F32), pl.BlockSpec((ONE, DC // SUB, SUB, SUB, LANE), o_map),
        grid=D // DC * n // C, flops=TWO * T * n * D, nbytes=T * D * THREE)


def dw1_kernel(*refs):
    a = jnp.concatenate([r[:] for r in refs[:-THREE]], axis=ONE)
    b_ref, _, o_ref = refs[-THREE:]
    r = dotg(a, b_ref[:], TN)
    for j in range(DC // LANE):
        o_ref[:, :, j] = r[:, LANE * j:LANE * (j + ONE)].reshape(o_ref.shape[:TWO] + (SUB, LANE))


def col_spec(k):
    return fixed((T, LANE), (ZERO, k), True)


def dw1_call(n2, dh, g, h=None):
    full = h is None
    own = ND // TWO
    specs = [fixed((T, C), once=True)] if full else [col_spec(TWO * k + h) for k in range(own)]
    rb = 32 if full else 16
    na = len(specs)
    shape = (ND, rb, 32, SUB, LANE)
    return run(dw1_kernel, (n2,) * na + (dh, g.reshape(shape)), specs + [pl.BlockSpec((T, DC), lambda i: (ZERO, i)), HBM],
        sds(shape, F32), pl.BlockSpec((own, rb, DC // LANE, SUB, LANE), lambda i: (ZERO, ZERO, i, ZERO, ZERO)), alias={na + ONE: ZERO},
        grid=D // DC, flops=TWO * T * (rb * 32) * D, nbytes=T * D * THREE)


def head_kernel(*refs):
    wall_ref, pooled_ref, bias_ref, lab_ref, dl_ref, gb_ref, loss_ref, dpool_ref, pall_ref, sqh_ref, w, lg, pb, st, sta, dps, dpr, ws, ss, rs, ss2, rs2, ss3, rs3 = refs
    for i in range(B // TWO):
        pb[TWO * i:TWO * i + TWO, :] = pooled_ref[i].astype(BF)
    row0 = pl.multiple_of(KC * lax.axis_index(AX), KC)
    cw = [pltpu.make_async_copy(wall_ref.at[r, pl.ds(row0, KC)], w.at[r], ws.at[r]) for r in range(ND)]
    for c in cw:
        c.start()
    me = entry_barrier()
    cs = ag_all(me, pb, pall_ref, ss, rs)
    pall_ref[me] = pb[:]
    wait_all(cs)

    wait_all(cw)
    bt = bias_ref[:].T
    pm = pall_ref[:].reshape(NIMG, C)
    for q in range(KR // TWO):
        n = q * TWO * LANE
        acc = jnp.concatenate([jnp.broadcast_to(bt[:, TWO * q + k:TWO * q + k + ONE], (LANE, NIMG)) for k in range(TWO)], axis=ZERO)
        acc = acc + dotg(jnp.concatenate([w[r, n:n + TWO * LANE, :] for r in range(ND)], axis=ONE), pm, NT)
        cls = KC * me + n + lax.broadcasted_iota(jnp.int32, (TWO * LANE, NIMG), ZERO)
        lg[n:n + TWO * LANE, :] = jnp.where(cls < NCLS, acc, -1e30)
    lab = lab_ref[ZERO:ONE, :].astype(jnp.int32)
    lgv = lg[:]
    hit = KC * me + lax.broadcasted_iota(jnp.int32, (KC, NIMG), ZERO) == lab
    m = jnp.max(lgv, axis=ZERO, keepdims=True)
    st[ZERO:ONE, :] = m
    st[ONE:TWO, :] = jnp.sum(jnp.exp(lgv - m), axis=ZERO, keepdims=True)
    st[TWO:THREE, :] = jnp.sum(jnp.where(hit, lgv, 0.0), axis=ZERO, keepdims=True)
    st[THREE:, :] = jnp.zeros((SUB - THREE, NIMG), F32)
    cs = ag_all(me, st, sta, ss2, rs2)
    sta[me] = st[:]
    wait_all(cs)
    top = sta[ZERO, ZERO:ONE, :]
    for k in range(ONE, ND):
        top = jnp.maximum(top, sta[k, ZERO:ONE, :])
    z = jnp.zeros((ONE, NIMG), F32)
    picked = jnp.zeros((ONE, NIMG), F32)
    for k in range(ND):
        z = z + sta[k, ONE:TWO, :] * jnp.exp(sta[k, ZERO:ONE, :] - top)
        picked = picked + sta[k, TWO:THREE, :]
    logz = top + jnp.log(z)
    loss_ref[:] = jnp.broadcast_to(jnp.sum(logz - picked, axis=ONE, keepdims=True) * (1.0 / NIMG), (SUB, LANE))
    gb_ref[:] = jnp.zeros(gb_ref.shape, F32)
    for q in range(KR):
        n = q * LANE
        hit = KC * me + n + lax.broadcasted_iota(jnp.int32, (LANE, NIMG), ZERO) == lab
        d = (jnp.exp(lg[n:n + LANE, :] - logz) - jnp.where(hit, 1.0, 0.0)) * (1.0 / NIMG)
        dl_ref[n:n + LANE, :] = d.astype(BF)
        gb_ref[q:q + ONE, :] = jnp.sum((d[:, :LANE] + d[:, LANE:]).T, axis=ZERO, keepdims=True)
    for r in range(ZERO, ND, TWO):
        dp = dotg(dl_ref[:], jnp.concatenate([w[r], w[r + ONE]], axis=ONE), TN)
        dps[:, :, r * LANE:(r + TWO) * LANE] = dp.reshape(ND, B, TWO * LANE)
    cs = []
    for d in range(ONE, ND):
        peer = lax.rem(me + d, ND)
        c = rcopy(dps.at[peer], dpr.at[me], ss3.at[d], rs3.at[d], peer)
        c.start()
        cs.append(c)
    dpr[me] = dps[me]
    gram = dotg(pm, pm, NT) * dotg(dl_ref[:], dl_ref[:], TN)
    sqh_ref[:] = sum8(gram[:, :LANE] + gram[:, LANE:])
    wait_all(cs)
    acc = dpr[ZERO]
    for k in range(ONE, ND):
        acc = acc + dpr[k]
    for i in range(B // TWO):
        dpool_ref[i] = acc[TWO * i:TWO * i + TWO]


def head(wall, pooled, wp, cid):
    n = (ND,)
    return run(head_kernel, (wall, pooled, wp[7], wp[6]), [HBM] + [VM] * THREE,
        [sds((KC, NIMG), BF), sds((24, LANE), F32), sds((SUB, LANE), F32), sds((B // TWO, TWO, C), F32), sds((ND, B, C), BF), sds((SUB, LANE), F32)], [VM] * 6,
        scratch=[pltpu.VMEM((ND, KC, LANE), BF), pltpu.VMEM((KC, NIMG), F32), pltpu.VMEM((B, C), BF), pltpu.VMEM((SUB, NIMG), F32), pltpu.VMEM((ND, SUB, NIMG), F32), pltpu.VMEM((ND, B, C), F32), pltpu.VMEM((ND, B, C), F32)] + [SEM(n)] * 7,
        flops=TWO * TEN**TEN, cid=cid)


def pack_small(dst, dw1_ref, dw2_ref, dbt1_ref, dbt2_ref, dg1_ref, ds1_ref, dg2_ref, ds2_ref, dbc1_ref, dbc2_ref, ws, wl, wh, xs):
    ws[:] = jnp.zeros(ws.shape, F32)
    ws[:, :SP] = dw1_ref[:]
    w1 = ws[:].T
    for j in range(FOUR):
        dst(j, S, FOUR, w1[:S, j * LANE:(j + ONE) * LANE])
    wl[:] = dw2_ref[:, :LANE]
    wh[:, :SP - LANE] = dw2_ref[:, LANE:]
    lane = lax.broadcasted_iota(jnp.int32, (16, LANE), ONE)
    for i in range(49):
        j0 = LANE * i // S
        s0 = LANE * i % S
        lo = wl[pl.ds(j0, 16, stride=32), :]
        hi = wh[pl.ds(j0, 16, stride=32), :]
        if s0 < LANE:
            v = shift_pick(lo, hi, lane, s0)
        else:
            v = pltpu.roll(hi, (TWO * LANE - s0) % LANE, ONE)
        left = S - s0
        if left < LANE:
            nx = wl[pl.ds(j0 + ONE, 16, stride=32), :]
            v = jnp.where(lane < left, v, pltpu.roll(nx, left, ONE))
        dst(HTOK + i, 16, 49, v)
    xs[:] = jnp.zeros(xs.shape, F32)

    def put(r0, v, n):
        for i in range(n):
            xs[r0 + i:r0 + i + ONE, :] = v[:, i * LANE:(i + ONE) * LANE]

    def tot(ref):
        return jnp.sum(ref[:], axis=ZERO, keepdims=True)

    put(ZERO, tot(dg2_ref), SUB)
    put(SUB, tot(ds2_ref), SUB)
    put(16, tot(dbc1_ref), 32)
    put(48, tot(dbc2_ref), SUB)
    x = xs[:]
    r = S - LANE
    lane8 = lax.broadcasted_iota(jnp.int32, (SMR, LANE), ONE)
    xr = pltpu.roll(x, r, ONE)
    xs[:] = jnp.zeros(xs.shape, F32)
    xs[21:77, :] = xr[:56]
    shifted = jnp.where(lane8 >= r, xs[:], 0.0)
    xs[22:78, :] = xr[:56]
    low = jnp.where(lane8 < r, xs[:], 0.0)
    row_i = lax.broadcasted_iota(jnp.int32, (SMR, LANE), ZERO)
    xs[:] = shifted + jnp.where(row_i >= 22, low, 0.0)
    put(ZERO, tot(dg1_ref), SUB)
    put(SUB, tot(ds1_ref), SUB)
    put(16, jnp.sum(dbt1_ref[:].T, axis=ZERO, keepdims=True), FOUR)
    bt2 = jnp.sum(dbt2_ref[:].T, axis=ZERO, keepdims=True)
    xs[20:21, :] = bt2[:, :LANE]
    xs[21:22, :r] = bt2[:, LANE:S]
    dst(TOKR, SMR, ONE, xs[:])
    dst(TOKR + SMR, ND * TP - TOKR - SMR, ONE, jnp.zeros((ND * TP - TOKR - SMR, LANE), F32))


PACK_SCR = [pltpu.VMEM((J, 256), F32), pltpu.VMEM((J, LANE), F32), pltpu.VMEM((J, LANE), F32), pltpu.VMEM((SMR, LANE), F32)]


def pack_kernel(extra, *refs):
    ins = refs[:TEN]
    o_ref, ws, wl, wh, xs = refs[-5:]

    def dst(r0, n, stride, v):
        if stride == ONE:
            o_ref[r0:r0 + n, :] = v
        else:
            o_ref[pl.ds(r0, n, stride=stride), :] = v

    pack_small(dst, *ins, ws, wl, wh, xs)
    if not extra:
        return
    gb_ref, dgf_ref, dsf_ref = refs[TEN:13]
    me = lax.axis_index(AX)
    base = ND * TP
    o_ref[base:, :] = jnp.zeros((SMF, LANE), F32)
    for r0, ref in ((ZERO, dgf_ref), (SUB, dsf_ref)):
        v = jnp.sum(ref[:], axis=ZERO, keepdims=True)
        for i in range(SUB):
            o_ref[base + r0 + i:base + r0 + i + ONE, :] = v[:, i * LANE:(i + ONE) * LANE]
    o_ref[pl.ds(base + 16 + KR * me, KR), :] = gb_ref[:KR, :]


def pack(parts, extra=()):
    ins = tuple(parts) + extra
    rows = ND * TP + (SMF if extra else ZERO)
    return run(functools.partial(pack_kernel, bool(extra)), ins, [VM] * len(ins), sds((rows, LANE), F32), VM, scratch=PACK_SCR)


def untile(g_ref, o_ref, me, r0=ZERO):
    off = TOKR - STEPR * me + r0

    def go(nj, acc0):
        def step(i, acc):
            for j in range(nj):
                v = g_ref[i * nj + j]
                o_ref[pl.ds(off + i * SUB * nj + j, SUB, stride=nj), :] = v
                acc = acc + v * v
            return acc

        return lax.fori_loop(ZERO, g_ref.shape[ZERO] // nj, step, acc0)

    return go


def fin_kernel(g_ref, tot_ref, sqh_ref, o_ref, sg_ref, sq_ref, sp_ref):
    me = lax.axis_index(AX)
    go = untile(g_ref, o_ref, me)
    base = ND * TP
    sg = tot_ref[pl.ds(pl.multiple_of(base + SMD * me, SUB), SMD), :]
    sg_ref[:] = sg
    tl = tot_ref[:base, :]
    acc = sqh_ref[:] + sum8(sg * sg) + jnp.where(me == ZERO, 1.0, 0.0) * sum8(tl * tl)

    @on(me < ND // TWO)
    def _():
        sq_ref[:] = go(D // LANE, acc)

    @on(me >= ND // TWO)
    def _():
        sq_ref[:] = go(C // LANE, acc)

    sp_ref[:] = o_ref[RSH:RSH + SPR, :]


def fin(g, tot, sqh):
    return run(fin_kernel, (g, tot, sqh), [VM] * THREE, [sds((GROWS, LANE), F32), sds((SMD, LANE), F32), sds((SUB, LANE), F32), sds((SPR, LANE), F32)], [VM] * FOUR)


def finh_kernel(g_ref, sqi_ref, o_ref, sq_ref, sp_ref):
    me = lax.axis_index(AX)
    go = untile(g_ref, o_ref, me, UR // TWO)

    @on(me < ND // TWO)
    def _():
        sq_ref[:] = go(D // LANE, sqi_ref[:])

    @on(me >= ND // TWO)
    def _():
        sq_ref[:] = go(C // LANE, sqi_ref[:])

    sp_ref[:] = o_ref[RSH:RSH + SPR, :]


def finh(g, sqi):
    return run(finh_kernel, (g, sqi), [VM] * TWO, [sds((GROWS, LANE), F32), sds((SUB, LANE), F32), sds((SPR, LANE), F32)], [VM] * THREE)


def tail_kernel(xb, g_ref, sqi_ref, gl_ref, o_ref, sca_ref, rb, sb, sqb, sqa, ss, rs, ss2, rs2, ss5, rs5, ss7, rs7):
    me = entry_barrier()

    def part(q):
        return xb.at[pl.ds(pl.multiple_of(q * TP, SUB), TP)]

    cs = []
    for d in range(ONE, ND):
        peer = lax.rem(me + d, ND)
        c = rcopy(part(peer), rb.at[me], ss.at[d], rs.at[d], peer)
        c.start()
        cs.append(c)
    rb[me] = xb[pl.ds(pl.multiple_of(me * TP, SUB), TP), :]
    go = untile(g_ref, gl_ref, me)

    @on(me < ND // TWO)
    def _():
        sqb[:] = go(D // LANE, sqi_ref[:])

    @on(me >= ND // TWO)
    def _():
        sqb[:] = go(C // LANE, sqi_ref[:])

    wait_all(cs)
    a = rb[ZERO]
    for k in range(ONE, ND):
        a = a + rb[k]
    sb[:] = a
    sqb[:] += sum8(a * a)
    csq = ag_all(me, sqb, sqa, ss7, rs7)
    sqa[me] = sqb[:]

    def to_first():
        return rcopy(sb, o_ref.at[me], ss2, rs2.at[me], ZERO)

    def to_last():
        return rcopy(sb, o_ref.at[me], ss5, rs5.at[me], ND - ONE)

    @on(me != ZERO)
    def _():
        to_first().start()

    @on(me != ND - ONE)
    def _():
        to_last().start()

    o_ref[me] = sb[:]
    wait_all(csq)
    t = sqa[ZERO]
    for k in range(ONE, ND):
        t = t + sqa[k]
    t = jnp.sum(jnp.sum(t, axis=ZERO, keepdims=True), axis=ONE, keepdims=True)
    sca_ref[:] = jnp.broadcast_to(1.0 / jnp.maximum(1.0, jnp.sqrt(t)), (SUB, LANE))

    @on(me != ZERO)
    def _():
        to_first().wait_send()

    @on(me != ND - ONE)
    def _():
        to_last().wait_send()

    @on(me == ZERO)
    def _():
        for d in range(ONE, ND):
            rcopy(sb, o_ref.at[d], ss2, rs2.at[d], ZERO).wait_recv()

    @on(me == ND - ONE)
    def _():
        for d in range(ND - ONE):
            rcopy(sb, o_ref.at[d], ss5, rs5.at[d], ZERO).wait_recv()


def tail(x, g, sqi, cid):
    n = (ND,)
    return run(tail_kernel, (x, g, sqi), [VM] * THREE,
        [sds((TOKR + UR // TWO + SUB, LANE), F32), sds((ND, TP, LANE), F32), sds((SUB, LANE), F32)], [VM] * THREE,
        scratch=[pltpu.VMEM((ND, TP, LANE), F32), pltpu.VMEM((TP, LANE), F32), pltpu.VMEM((SUB, LANE), F32), pltpu.VMEM((ND, SUB, LANE), F32),
            SEM(n), SEM(n), SEM, SEM(n), SEM, SEM(n), SEM(n), SEM(n)], cid=cid, vlim=VTAIL, flops=40 * TEN**9)


def adam_math(p, m, v, g, decay):
    m2 = BETA_ONE * m + (1.0 - BETA_ONE) * g
    v2 = BETA_TWO * v + (1.0 - BETA_TWO) * g * g
    mh = m2 * (1.0 / (1.0 - BETA_ONE ** ADAM_STEP))
    vh = v2 * (1.0 / (1.0 - BETA_TWO ** ADAM_STEP))
    return p - LEARN_RATE * (mh / (jnp.sqrt(vh) + ADAM_EPS) + decay * p), m2, v2


ABR = 2800
HAA = 5632
NAB = -(-RSH // ABR)


def head_adam_kernel(sc_ref, dl_ref, pc_ref, p_ref, m_ref, v_ref, po_ref, mo_ref, vo_ref):
    g = dot(dl_ref[:], pc_ref[:]) * sc_ref[ZERO, ZERO]
    po_ref[:], mo_ref[:], vo_ref[:] = adam_math(p_ref[:], m_ref[:], v_ref[:], g, WEIGHT_DECAY)


def head_adam(sc, dl, pc, p, m, v):
    blk = pl.BlockSpec((HAA, LANE), lambda i: (i, ZERO))
    return run(head_adam_kernel, (sc, dl, pc, p, m, v), [SMEM, pl.BlockSpec((HAA, NIMG), lambda i: (i, ZERO)), fixed((NIMG, LANE)), blk, blk, blk],
        [sds(p.shape, F32)] * THREE, [blk] * THREE, grid=-(-NCLS // HAA), flops=30 * TEN**9, nbytes=8 * TEN**7)


def layer_adam_kernel(sc_ref, g0_ref, h0_ref, g1_ref, t0_ref, t1_ref, s0_ref, s1_ref, p_ref, m_ref, v_ref, po_ref, mo_ref, vo_ref, gs):
    k = lax.axis_index(AX)
    i = pl.program_id(ZERO)
    off = TOKR - STEPR * k
    sc = sc_ref[ZERO, ZERO]
    lays = ((g0_ref, t0_ref, s0_ref), (g1_ref, t1_ref, s1_ref))
    ri = i * ABR + lax.broadcasted_iota(jnp.int32, (ABR, LANE), ZERO)
    gs[pl.ds(ZERO, ABR, stride=TWO), :] = jnp.where(ri < off + UR // TWO, g0_ref[:], h0_ref[:]) * sc
    gs[pl.ds(ONE, ABR, stride=TWO), :] = g1_ref[:] * sc
    for b in range(-(-TOKR // ABR)):
        @on(i == b)
        def _():
            n = min(ABR, TOKR - b * ABR)
            r = b * ABR + lax.broadcasted_iota(jnp.int32, (n, LANE), ZERO)
            for l in range(TWO):
                g_ref, t_ref, s_ref = lays[l]
                e = min(n, SPR - b * ABR)
                sp = s_ref[b * ABR:b * ABR + e, :]
                if e < n:
                    sp = jnp.concatenate([sp, jnp.zeros((n - e, LANE), F32)], axis=ZERO)
                alt = jnp.where(k == ZERO, t_ref[b * ABR:b * ABR + n, :], sp)
                gs[pl.ds(l, n, stride=TWO), :] = jnp.where(r < off, alt, g_ref[:n, :]) * sc

    @on(jnp.logical_and(i == NAB - ONE, k == ND - ONE))
    def _():
        r0 = RSH - SMR - (NAB - ONE) * ABR
        for l in range(TWO):
            gs[pl.ds(TWO * r0 + l, SMR, stride=TWO), :] = lays[l][ONE][TOKR:TOKR + SMR, :] * sc

    n2 = TWO * ABR
    r2 = TWO * (RSH * k + i * ABR) + lax.broadcasted_iota(jnp.int32, (n2, LANE), ZERO)
    decay = jnp.where(r2 < TWO * MATR, WEIGHT_DECAY, 0.0)
    a, b, c = adam_math(p_ref.reshape(n2, LANE)[:], m_ref.reshape(n2, LANE)[:], v_ref.reshape(n2, LANE)[:], gs[:], decay)
    po_ref.reshape(n2, LANE)[:] = a
    mo_ref.reshape(n2, LANE)[:] = b
    vo_ref.reshape(n2, LANE)[:] = c


def layer_adam(sc, g0, h0, g1, t0, t1, s0, s1, p, m, v):
    blk = pl.BlockSpec((ABR, TWO, LANE), lambda i: (i, ZERO, ZERO))
    gb = pl.BlockSpec((ABR, LANE), lambda i: (i, ZERO))
    return run(layer_adam_kernel, (sc, g0, h0, g1, t0, t1, s0, s1, p, m, v),
        [SMEM, gb, pl.BlockSpec((ABR, LANE), lambda i: (jnp.maximum(i, ONE), ZERO)), gb] + [fixed(t.shape) for t in (t0, t1, s0, s1)] + [blk] * THREE, [sds(p.shape, F32)] * THREE, [blk] * THREE,
        scratch=[pltpu.VMEM((TWO * ABR, LANE), F32)], grid=NAB, nbytes=6 * TEN**7)


def solution(mesh):
    row_spec = P(AX)
    layer_spec = P(None, AX)
    in_specs = (row_spec, row_spec, layer_spec, row_spec, row_spec, layer_spec, row_spec, row_spec, layer_spec, row_spec, row_spec)
    out_specs = (P(),) + in_specs[TWO:]
    up = [(i, (i + ONE) % ND) for i in range(ND)]

    def scatter(grad, n):
        return lax.psum_scatter(grad.reshape(ND, n, LANE), AX, scatter_dimension=ZERO, tiled=True).reshape(n // SUB, SUB, LANE)

    def device_step(act_in, labels, layer_p, head_w, small_p, layer_m, head_m, small_m, layer_v, head_v, small_v):
        me = lax.axis_index(AX)
        p3 = rows3(layer_p)
        lab = jnp.pad(labels.astype(F32)[None, :], ((ZERO, SUB - ONE), (ZERO, LANE - B)))
        misc = jnp.concatenate([small_p.reshape(SMD, LANE), lab], axis=ZERO)
        t0, t1, sh0, sh1, toks, tok1, sms, left0, left1 = prep(p3)
        sh1 = lax.ppermute(sh1, AX, [(b, a) for a, b in up])
        t0, tok0, sm_all, misc_all, hb = start(sh0, toks, sms, misc, left0, t0, head_w.T, ONE)
        t1 = fix(sh1, left1, t1)
        wg = []
        for t in (t0, t1):
            wg.append(lax.all_gather(t, AX, tiled=True))
        tok1 = lax.psum(tok1, AX)
        wp = [wprep(ZERO, tok0, sm_all, misc_all)]
        hidden = act_in
        saved = []
        for l in range(TWO):
            x1, n2, ta, tg = tok_fwd(hidden, wp[l])
            if l == ZERO:
                wall = lax.all_gather(hb, AX)
                wp.append(wprep(ONE, tok1, sm_all, misc_all))
            x1 = x1.reshape(T, C)
            n2 = n2.reshape(T, C)
            x2, act, gp, *pooled = ch_fwd(n2, x1, wg[l], wp[l], l)
            saved.append((hidden, ta, tg, x1, n2, act, gp))
            hidden = x2.reshape(B, SP, C)
        dl, gb, loss, dpool, pall, sqh = head(wall, pooled[ZERO], wp[ZERO], TWO)
        dl_all = lax.all_gather(dl, AX, tiled=True)
        pc = lax.dynamic_slice_in_dim(pall.reshape(NIMG, C), LANE * me, LANE, axis=ONE)
        for l in (ONE, ZERO):
            hid_in, ta, tg, x1, n2, act, gp = saved[l]
            if l:
                dh, dbc1, dbc2, d_out, dgf, dsf = ch_bwd_top(x2, dpool, gp, wg[l], wp[l])
                dh, dl_all = lax.optimization_barrier((dh, dl_all))
                grad = dw1_call(n2, dh, dw2_call(act, d_out))
                dh, grad = lax.optimization_barrier((dh, grad))
                shard1 = scatter(grad, UR)
            else:
                g2 = dw2_call(act, d_out, ONE)
                g2, d_out = lax.optimization_barrier((g2, d_out))
                dh, dbc1, dbc2 = ch_bwd_a(d_out, gp, wg[l])
                dh, tot = lax.optimization_barrier((dh, tot))
                grad = dw1_call(n2, dh, g2, ONE)
                dh, grad, tot, act = lax.optimization_barrier((dh, grad, tot, act))
                shard_b = scatter(grad, UR // TWO)
                gl1, small_g, sq, sp1 = fin(shard1, tot, sqh)
                sp1 = lax.ppermute(sp1, AX, up)
                dh, sq, act = lax.optimization_barrier((dh, sq, act))
                grad = dw1_call(n2, dh, dw2_call(act, d_out, ZERO), ZERO)
                dh, grad = lax.optimization_barrier((dh, grad))
                shard_a = scatter(grad, UR // TWO)
            da, dg2, ds2 = ch_bwd_b(dh, wg[l], x1, d_out, wp[l])
            if l == ZERO:
                h0, sq, sp0 = finh(shard_b, sq)
                sp0 = lax.ppermute(sp0, AX, up)
                da, sq = lax.optimization_barrier((da, sq))
            o = tok_bwd(hid_in, da.reshape(B, SP, C), ta, tg, wp[l], l)
            if l:
                d_out = o[ZERO].reshape(T, C)
                o = o[ONE:]
            parts = tuple(o) + (dg2, ds2, dbc1, dbc2)
            if l:
                sv, d_out = lax.optimization_barrier((pack(parts, (gb, dgf, dsf)), d_out))
                tot = lax.psum(sv, AX)
        px, sp0 = lax.optimization_barrier((pack(parts), sp0))
        gl0, tsm, sca = tail(px, shard_a, sq, FOUR)
        np3, nm3, nv3 = layer_adam(sca, gl0, h0, gl1, tsm.reshape(ND * TP, LANE), tot, sp0, sp1, p3, rows3(layer_m), rows3(layer_v))
        nh, nhm, nhv = head_adam(sca, dl_all, pc, head_w.T, head_m.T, head_v.T)
        nsp, nsm, nsv = adam_math(small_p, small_m, small_v, small_g.reshape(SMD * LANE) * sca[ZERO, ZERO], 0.0)
        return (loss[ZERO, ZERO], unrows3(np3), nh.T, nsp, unrows3(nm3), nhm.T, nsm, unrows3(nv3), nhv.T, nsv)

    return jax.shard_map(device_step, mesh=mesh, in_specs=in_specs, out_specs=out_specs, check_vma=False)
```
